16 devices in a mesh: rep: 1, r: 2 (over z), s: 8 (over x, y, core).
Axes of the slice: x: 2, y: 2, z: 2, core: 2. Of those that a mesh axis runs over, the one named last changes fastest.
Arguments:
- x: bfloat16 [16, 4096, 896], P(('rep', 'r', 's'))
- dy: bfloat16 [16, 4096, 896], P(('rep', 'r', 's'))
- w_gate: bfloat16 [2, 896, 2560], P(None, 's')
- w_up: bfloat16 [2, 896, 2560], P(None, 's')
- w_down: bfloat16 [2, 2560, 896], P(None, 's')
- m_w_gate: float32 [2, 896, 2560], P(None, 's')
- m_w_up: float32 [2, 896, 2560], P(None, 's')
- m_w_down: float32 [2, 2560, 896], P(None, 's')
- v_w_gate: float32 [2, 896, 2560], P(None, 's')
- v_w_up: float32 [2, 896, 2560], P(None, 's')
- v_w_down: float32 [2, 2560, 896], P(None, 's')
Outputs:
- output 1: bfloat16 [2, 896, 2560], P('rep', 's')
- output 2: bfloat16 [2, 896, 2560], P('rep', 's')
- output 3: bfloat16 [2, 2560, 896], P('rep', 's')
- output 4: float32 [2, 896, 2560], P('rep', 's')
- output 5: float32 [2, 896, 2560], P('rep', 's')
- output 6: float32 [2, 2560, 896], P('rep', 's')
- output 7: float32 [2, 896, 2560], P('rep', 's')
- output 8: float32 [2, 896, 2560], P('rep', 's')
- output 9: float32 [2, 2560, 896], P('rep', 's')
All inputs are finite; a program needn't handle non-finite values.
Results may differ from the reference program's by a relative error of at most 0.022.
Values are sent between devices in bfloat16 or wider.
A program may use at most 2 GiB of HBM per device.

```python
import jax
import jax.numpy as jnp
from jax import lax

SEQUENCES = 16
TOKENS = 4096
D = 896
FF = 2560
LAYERS = 2
NAMES = ("w_gate", "w_up", "w_down")
SHAPES = {"w_gate": (LAYERS, D, FF), "w_up": (LAYERS, D, FF), "w_down": (LAYERS, FF, D)}


def bump(key, n, height):
    away = (jnp.arange(n, dtype=jnp.int32) - jax.random.randint(key, (), 0, n, jnp.int32)) % n
    return jnp.where(away < n // 8, height, 1.0)


def together(key, own, strength):
    shared = jax.random.normal(key, own.shape[1:], jnp.float32)
    return (own + strength * shared) * lax.rsqrt(1 + strength * strength)


def setup_inputs(seed: int = 0, part: int = 0) -> dict:
    kx, kdy, ka, kb, kz, kf, kh, kl, *keys = jax.random.split(jax.random.key(seed), 8 + 3 * len(NAMES))
    kx, kdy, ka, kb = (jax.random.fold_in(k, part) for k in (kx, kdy, ka, kb))
    kw, km, kv = (keys[i::3] for i in range(3))
    shape = (SEQUENCES, TOKENS, D)
    much_x, much_dy = jax.random.uniform(kz, (2,), jnp.float32, 0.0, 1.0)
    loud = 2.0 ** jax.random.uniform(jax.random.fold_in(kz, 1), (), jnp.float32, -1.0, 2.0)
    layers = 2.0 ** jax.random.uniform(kl, (LAYERS, 1, 1), jnp.float32, -1.0, 1.0)
    x = together(ka, jax.random.normal(kx, shape, jnp.float32), much_x) * bump(kf, D, 4.0)
    dy = together(kb, jax.random.normal(kdy, shape, jnp.float32), much_dy)
    drawn = {"x": x.astype(jnp.bfloat16), "dy": (loud * dy * (SEQUENCES * TOKENS) ** -0.5).astype(jnp.bfloat16)}
    for key, name in zip(kw, NAMES, strict=True):
        w = jax.random.normal(key, SHAPES[name], jnp.float32) * SHAPES[name][1] ** -0.5
        drawn[name] = (w * {"w_gate": 1.0, "w_up": bump(kh, FF, 4.0), "w_down": layers}[name]).astype(jnp.bfloat16)
    for key, name in zip(km, NAMES, strict=True):
        drawn[f"m_{name}"] = 0.1 * jax.random.normal(key, SHAPES[name], jnp.float32)
    for key, name in zip(kv, NAMES, strict=True):
        drawn[f"v_{name}"] = jax.random.uniform(key, SHAPES[name], jnp.float32, 0.005, 0.015)
    return drawn


def matmul(a, w):
    return jnp.dot(a, w, preferred_element_type=jnp.float32).astype(jnp.bfloat16)


def normed(h):
    wide = h.astype(jnp.float32)
    scale = lax.rsqrt(jnp.mean(wide**2, -1, keepdims=True) + 1e-6)
    return (wide * scale).astype(jnp.bfloat16)


def layer(h, w):
    a = normed(h)
    gate = jnp.dot(a, w["w_gate"], preferred_element_type=jnp.float32)
    up = jnp.dot(a, w["w_up"], preferred_element_type=jnp.float32)
    return h + matmul((jax.nn.silu(gate) * up).astype(jnp.bfloat16), w["w_down"])


def adamw(w, m, v, g):
    m = 0.9 * m + 0.1 * g
    v = 0.95 * v + 0.05 * g * g
    step = m * lax.rsqrt(v + 1e-8) + 0.1 * w
    return (w - 0.02 * step).astype(jnp.bfloat16), m, v


def clipped(gradients, sum_of_squares, count):
    factor = jnp.minimum(1.0, 0.5 * lax.rsqrt(sum_of_squares / count + 1e-30))
    return [g * factor for g in gradients]


def stack(weights, h):
    return lax.scan(lambda h, w: (layer(h, w), None), h, weights)[0]


def reference(x, dy, w_gate, w_up, w_down, m_w_gate, m_w_up, m_w_down, v_w_gate, v_w_up, v_w_down):
    weights = dict(zip(NAMES, (w_gate, w_up, w_down), strict=True))

    def take(so_far, sequence):
        h, by_y = sequence
        _, back = jax.vjp(lambda w: stack(w, h), weights)
        return jax.tree.map(lambda total, term: total + term.astype(jnp.float32), so_far, back(by_y)[0]), None

    none_yet = {name: jnp.zeros(w.shape, jnp.float32) for name, w in weights.items()}
    by_weights, _ = lax.scan(take, none_yet, (x, dy))
    gradients = [by_weights[name].astype(jnp.bfloat16).astype(jnp.float32) for name in NAMES]
    gradients = clipped(gradients, sum(jnp.sum(g * g) for g in gradients), sum(g.size for g in gradients))
    new = [
        adamw(w.astype(jnp.float32), m, v, g)
        for w, m, v, g in zip((w_gate, w_up, w_down), (m_w_gate, m_w_up, m_w_down), (v_w_gate, v_w_up, v_w_down), gradients, strict=True)
    ]
    return tuple(one[which] for which in range(3) for one in new)
```

```python
import functools

import jax
import jax.numpy as jnp
from jax import lax
from jax.experimental import pallas as pl
from jax.experimental.pallas import tpu as pltpu
from jax.sharding import PartitionSpec as P

NAMES = ("w_gate", "w_up", "w_down")
bf16, f32 = jnp.bfloat16, jnp.float32
CH, SUB, TM, LANES = 256, 512, 1024, 128
NT_DIMS = (((1,), (1,)), ((), ()))
TN_DIMS = (((0,), (0,)), ((), ()))
VMEM_LIMIT = 67043328


def groups_of(i):
    j, half = i // 2, i % 2
    first = j + 10 * half
    return first * LANES, (first + 5) * LANES


def dot(a, b):
    return jnp.dot(a, b, preferred_element_type=f32)


def rows_at(start, size, multiple=None):
    return pl.ds(pl.multiple_of(start, multiple or size), size)


def sigmoid(x):
    return 1.0 / (1.0 + jnp.exp(-x))


def columns_in(w_hbm, buf, sem, i, offset):
    return [
        pltpu.make_async_copy(w_hbm.at[:, rows_at(start, LANES)], buf.at[:, pl.ds(offset + LANES * n, LANES)], sem.at[n])
        for n, start in enumerate(groups_of(i))
    ]


def rows_in(w_hbm, buf, sem, i):
    return [
        pltpu.make_async_copy(w_hbm.at[rows_at(start, LANES), :], buf.at[pl.ds(LANES * n, LANES), :], sem.at[n])
        for n, start in enumerate(groups_of(i))
    ]


def start(copies):
    for c in copies:
        c.start()


def wait(copies):
    for c in copies:
        c.wait()


def normed_in_place(a_ref, aT_ref, t):
    rows = rows_at(t * 256, 256)
    w = a_ref[rows, :].astype(f32)
    a = (w * lax.rsqrt(jnp.mean(w * w, -1, keepdims=True) + 1e-6)).astype(bf16)
    a_ref[rows, :] = a
    if aT_ref is not None:
        aT_ref[:, rows] = a.T


def forward_kernel(h_hbm, wg_hbm, wu_hbm, wd_hbm, gu_hbm, out_hbm, a_ref, act_ref, wgu, wd, gus, hin, hout, hsem, wsem, wdsem, gsem, xsem, osem):
    T, D = a_ref.shape
    F = act_ref.shape[1]
    NC, NT = F // CH, T // TM

    def loads(t):
        rows = rows_at(t * 256, 256)
        return [pltpu.make_async_copy(h_hbm.at[rows, :], a_ref.at[rows, :], hsem.at[t])]

    def weights(i):
        slot = i % 2
        return columns_in(wg_hbm, wgu.at[slot], wsem.at[slot, 0], i, 0) + columns_in(wu_hbm, wgu.at[slot], wsem.at[slot, 1], i, CH)

    def saves(n):
        i, t = n // NT, n % NT
        return [pltpu.make_async_copy(gus.at[n % 2], gu_hbm.at[i, rows_at(t * TM, TM), :], gsem.at[n % 2])]

    def downs(i):
        return rows_in(wd_hbm, wd.at[rows_at(i * CH, CH), :], wdsem.at[i], i)

    lax.fori_loop(0, T // 256, lambda t, _: start(loads(t)) or 0, 0)
    start(weights(0))

    def norm(t, _):
        wait(loads(t))
        normed_in_place(a_ref, None, t)
        return 0

    lax.fori_loop(0, T // 256, norm, 0)
    lax.fori_loop(0, NC, lambda i, _: start(downs(i)) or 0, 0)

    def chunk(i, _):
        slot = i % 2
        wait(weights(i))

        @pl.when(i + 1 < NC)
        def _():
            start(weights(i + 1))

        def tile(t, _):
            n = i * NT + t

            @pl.when(n >= 2)
            def _():
                wait(saves(n - 2))

            def dots(k):
                gu = dot(a_ref[rows_at(t * TM + k * SUB, SUB), :], wgu[slot])
                gus[n % 2, pl.ds(k * SUB, SUB), :] = gu
                return gu

            def elementwise(k, gu):
                gate, up = gu[:, :CH], gu[:, CH:]
                act_ref[rows_at(t * TM + k * SUB, SUB), rows_at(i * CH, CH)] = (gate * sigmoid(gate) * up).astype(bf16)

            gu = dots(0)
            for k in range(TM // SUB):
                following = dots(k + 1) if k + 1 < TM // SUB else None
                elementwise(k, gu)
                gu = following
            start(saves(n))
            return 0

        lax.fori_loop(0, NT, tile, 0)
        return 0

    lax.fori_loop(0, NC, chunk, 0)
    lax.fori_loop(0, NC, lambda i, _: wait(downs(i)) or 0, 0)

    def inputs(t):
        return [pltpu.make_async_copy(h_hbm.at[rows_at(t * SUB, SUB), :], hin.at[t % 2], xsem.at[t % 2])]

    def outputs(t):
        return [pltpu.make_async_copy(hout.at[t % 2], out_hbm.at[rows_at(t * SUB, SUB), :], osem.at[t % 2])]

    start(inputs(0))

    def down(t, _):
        wait(inputs(t))

        @pl.when(t + 1 < T // SUB)
        def _():
            start(inputs(t + 1))

        @pl.when(t >= 2)
        def _():
            wait(outputs(t - 2))

        out = dot(act_ref[rows_at(t * SUB, SUB), :], wd[...]).astype(bf16)
        hout[t % 2] = (hin[t % 2].astype(f32) + out.astype(f32)).astype(bf16)
        start(outputs(t))
        return 0

    lax.fori_loop(0, T // SUB, down, 0)
    for n in (NC * NT - 2, NC * NT - 1):
        wait(saves(n))
    for t in (T // SUB - 2, T // SUB - 1):
        wait(outputs(t))


def middle_kernel(h_hbm, dy_hbm, wg_hbm, wu_hbm, wd_hbm, dwg_hbm, dwu_hbm, dwd_hbm, dh_hbm,
                  a_ref, aT_ref, dy_ref, da_ref, dgu_ref, act_ref, wgu, wd, ob, obd, hsem, ysem, wsem, osem):
    T, D = a_ref.shape
    F = dwg_hbm.shape[1]
    NC, NT = F // CH, T // TM

    def loads(t):
        rows = rows_at(t * 256, 256)
        return [pltpu.make_async_copy(h_hbm.at[rows, :], a_ref.at[rows, :], hsem.at[t])]

    def dys():
        return [pltpu.make_async_copy(dy_hbm, dy_ref, ysem)]

    def weights(i):
        slot = i % 2
        return (
            columns_in(wg_hbm, wgu.at[slot], wsem.at[slot, 0], i, 0)
            + columns_in(wu_hbm, wgu.at[slot], wsem.at[slot, 1], i, CH)
            + rows_in(wd_hbm, wd.at[slot], wsem.at[slot, 2], i)
        )

    def outs(i):
        slot = i % 2
        copies = []
        for n, at in enumerate(groups_of(i)):
            cols = rows_at(at, LANES)
            copies += [
                pltpu.make_async_copy(ob.at[slot, :, pl.ds(LANES * n, LANES)], dwg_hbm.at[:, cols], osem.at[slot, 0, n]),
                pltpu.make_async_copy(ob.at[slot, :, pl.ds(CH + LANES * n, LANES)], dwu_hbm.at[:, cols], osem.at[slot, 1, n]),
                pltpu.make_async_copy(obd.at[slot, pl.ds(LANES * n, LANES), :], dwd_hbm.at[cols, :], osem.at[slot, 2, n]),
            ]
        return copies

    lax.fori_loop(0, T // 256, lambda t, _: start(loads(t)) or 0, 0)
    start(weights(0))
    start(dys())

    def norm(t, _):
        wait(loads(t))
        normed_in_place(a_ref, aT_ref, t)
        da_ref[rows_at(t * 256, 256), :] = jnp.zeros((256, D), f32)
        return 0

    lax.fori_loop(0, T // 256, norm, 0)
    wait(dys())

    def chunk(i, _):
        slot = i % 2
        wait(weights(i))

        @pl.when(i + 1 < NC)
        def _():
            start(weights(i + 1))

        def tile(t, _):
            def rows_of(k):
                return rows_at(t * TM + k * SUB, SUB)

            def dots(k):
                rows = rows_of(k)
                return dot(a_ref[rows, :], wgu[slot]), lax.dot_general(dy_ref[rows, :], wd[slot], NT_DIMS, preferred_element_type=f32)

            def elementwise(k, gu, dact):
                rows = rows_of(k)
                dact = dact.astype(bf16).astype(f32)
                gate, up = gu[:, :CH], gu[:, CH:]
                sg = sigmoid(gate)
                silu = gate * sg
                act_ref[rows, :] = (silu * up).astype(bf16)
                dgate = (dact * up * (sg * (1.0 + gate * (1.0 - sg)))).astype(bf16)
                dup = (dact * silu).astype(bf16)
                dgu_ref[rows, pl.ds(0, CH)] = dgate
                dgu_ref[rows, pl.ds(CH, CH)] = dup
                return jnp.concatenate([dgate, dup], 1)

            def back(k, dgu):
                da_ref[rows_of(k), :] += lax.dot_general(dgu, wgu[slot], NT_DIMS, preferred_element_type=f32)

            now, before = dots(0), None
            for k in range(TM // SUB):
                following = dots(k + 1) if k + 1 < TM // SUB else None
                dgu = elementwise(k, *now)
                if before is not None:
                    back(k - 1, before)
                before, now = dgu, following
            back(TM // SUB - 1, before)
            return 0

        lax.fori_loop(0, NT, tile, 0)

        @pl.when(i >= 2)
        def _():
            wait(outs(i - 2))

        ob[slot] = dot(aT_ref[...], dgu_ref[...]).astype(bf16)
        obd[slot] = lax.dot_general(act_ref[...], dy_ref[...], TN_DIMS, preferred_element_type=f32).astype(bf16)
        start(outs(i))
        return 0

    lax.fori_loop(0, NC, chunk, 0)
    lax.fori_loop(0, T // 256, lambda t, _: start(loads(t)) or 0, 0)

    def stores(t):
        rows = rows_at(t * 256, 256)
        return [pltpu.make_async_copy(dy_ref.at[rows, :], dh_hbm.at[rows, :], hsem.at[t])]

    def norm_back(t, _):
        rows = rows_at(t * 256, 256)
        wait(loads(t))
        w = a_ref[rows, :].astype(f32)
        da = da_ref[rows, :].astype(bf16).astype(f32)
        scale = lax.rsqrt(jnp.mean(w * w, -1, keepdims=True) + 1e-6)
        along = jnp.sum(da * w, -1, keepdims=True) * (scale * scale * scale) * (1.0 / D)
        by_h = (da * scale - w * along).astype(bf16)
        dy_ref[rows, :] = (dy_ref[rows, :].astype(f32) + by_h.astype(f32)).astype(bf16)
        start(stores(t))
        return 0

    lax.fori_loop(0, T // 256, norm_back, 0)
    lax.fori_loop(0, T // 256, lambda t, _: wait(stores(t)) or 0, 0)
    for i in (NC - 2, NC - 1):
        wait(outs(i))


def last_kernel(h_hbm, dy_hbm, gu_hbm, wd_hbm, dwg_hbm, dwu_hbm, dwd_hbm,
                a_ref, aT_ref, dy_ref, dgu_ref, act_ref, gus, wd, ob, obd, hsem, ysem, gsem, wsem, osem):
    T, D = a_ref.shape
    F = dwg_hbm.shape[1]
    NC, NT = F // CH, T // TM

    def loads(t):
        rows = rows_at(t * 256, 256)
        return [pltpu.make_async_copy(h_hbm.at[rows, :], a_ref.at[rows, :], hsem.at[t])]

    def dys():
        return [pltpu.make_async_copy(dy_hbm, dy_ref, ysem)]

    def weights(i):
        slot = i % 2
        return rows_in(wd_hbm, wd.at[slot], wsem.at[slot], i)

    def kept(n):
        i, t = n // NT, n % NT
        return [pltpu.make_async_copy(gu_hbm.at[i, rows_at(t * TM, TM), :], gus.at[n % 2], gsem.at[n % 2])]

    def outs(i):
        slot = i % 2
        copies = []
        for n, at in enumerate(groups_of(i)):
            cols = rows_at(at, LANES)
            copies += [
                pltpu.make_async_copy(ob.at[slot, :, pl.ds(LANES * n, LANES)], dwg_hbm.at[:, cols], osem.at[slot, 0, n]),
                pltpu.make_async_copy(ob.at[slot, :, pl.ds(CH + LANES * n, LANES)], dwu_hbm.at[:, cols], osem.at[slot, 1, n]),
                pltpu.make_async_copy(obd.at[slot, pl.ds(LANES * n, LANES), :], dwd_hbm.at[cols, :], osem.at[slot, 2, n]),
            ]
        return copies

    lax.fori_loop(0, T // 256, lambda t, _: start(loads(t)) or 0, 0)
    start(weights(0))
    start(dys())
    start(kept(0))

    def norm(t, _):
        wait(loads(t))
        normed_in_place(a_ref, aT_ref, t)
        return 0

    lax.fori_loop(0, T // 256, norm, 0)
    wait(dys())

    def chunk(i, _):
        slot = i % 2
        wait(weights(i))

        @pl.when(i + 1 < NC)
        def _():
            start(weights(i + 1))

        def tile(t, _):
            n = i * NT + t
            wait(kept(n))

            @pl.when(n + 1 < NC * NT)
            def _():
                start(kept(n + 1))

            def rows_of(k):
                return rows_at(t * TM + k * SUB, SUB)

            def dots(k):
                return lax.dot_general(dy_ref[rows_of(k), :], wd[slot], NT_DIMS, preferred_element_type=f32)

            def elementwise(k, dact):
                rows = rows_of(k)
                dact = dact.astype(bf16).astype(f32)
                gate, up = gus[n % 2, pl.ds(k * SUB, SUB), pl.ds(0, CH)], gus[n % 2, pl.ds(k * SUB, SUB), pl.ds(CH, CH)]
                sg = sigmoid(gate)
                silu = gate * sg
                act_ref[rows, :] = (silu * up).astype(bf16)
                dgu_ref[rows, pl.ds(0, CH)] = (dact * up * (sg * (1.0 + gate * (1.0 - sg)))).astype(bf16)
                dgu_ref[rows, pl.ds(CH, CH)] = (dact * silu).astype(bf16)

            now = dots(0)
            for k in range(TM // SUB):
                following = dots(k + 1) if k + 1 < TM // SUB else None
                elementwise(k, now)
                now = following
            return 0

        lax.fori_loop(0, NT, tile, 0)

        @pl.when(i >= 2)
        def _():
            wait(outs(i - 2))

        ob[slot] = dot(aT_ref[...], dgu_ref[...]).astype(bf16)
        obd[slot] = lax.dot_general(act_ref[...], dy_ref[...], TN_DIMS, preferred_element_type=f32).astype(bf16)
        start(outs(i))
        return 0

    lax.fori_loop(0, NC, chunk, 0)
    for i in (NC - 2, NC - 1):
        wait(outs(i))


def call(kernel, outs, scratch, inputs, **params):
    anywhere = pl.BlockSpec(memory_space=pl.ANY)
    return pl.pallas_call(
        kernel,
        out_shape=[jax.ShapeDtypeStruct(*o) for o in outs],
        in_specs=[anywhere] * len(inputs),
        out_specs=[anywhere] * len(outs),
        scratch_shapes=scratch,
        compiler_params=pltpu.CompilerParams(vmem_limit_bytes=VMEM_LIMIT, **params),
    )(*inputs)


def forward(h, wg, wu, wd):
    (T, D), F = h.shape, wg.shape[1]
    V, S = pltpu.VMEM, pltpu.SemaphoreType.DMA
    return call(
        forward_kernel,
        [((F // CH, T, 2 * CH), f32), ((T, D), bf16)],
        [V((T, D), bf16), V((T, F), bf16), V((2, D, 2 * CH), bf16), V((F, D), bf16), V((2, TM, 2 * CH), f32), V((2, SUB, D), bf16), V((2, SUB, D), bf16)]
        + [S((T // 256,)), S((2, 2, 2)), S((F // CH, 2)), S((2,)), S((2,)), S((2,))],
        (h, wg, wu, wd),
    )


def middle(h, dy, wg, wu, wd):
    (T, D), F = h.shape, wg.shape[1]
    V, S = pltpu.VMEM, pltpu.SemaphoreType.DMA
    return call(
        middle_kernel,
        [((D, F), bf16), ((D, F), bf16), ((F, D), bf16), ((T, D), bf16)],
        [V((T, D), bf16), V((D, T), bf16), V((T, D), bf16), V((T, D), f32), V((T, 2 * CH), bf16), V((T, CH), bf16)]
        + [V((2, D, 2 * CH), bf16), V((2, CH, D), bf16), V((2, D, 2 * CH), bf16), V((2, CH, D), bf16)]
        + [S((T // 256,)), S(()), S((2, 3, 2)), S((2, 3, 2))],
        (h, dy, wg, wu, wd),
    )


def last(h, dy, gu, wd):
    (T, D), F = h.shape, wd.shape[0]
    V, S = pltpu.VMEM, pltpu.SemaphoreType.DMA
    return call(
        last_kernel,
        [((D, F), bf16), ((D, F), bf16), ((F, D), bf16)],
        [V((T, D), bf16), V((D, T), bf16), V((T, D), bf16), V((T, 2 * CH), bf16), V((T, CH), bf16), V((2, TM, 2 * CH), f32)]
        + [V((2, CH, D), bf16), V((2, D, 2 * CH), bf16), V((2, CH, D), bf16)]
        + [S((T // 256,)), S(()), S((2,)), S((2, 2)), S((2, 3, 2))],
        (h, dy, gu, wd),
    )


def adamw(w, m, v, g):
    m = 0.9 * m + 0.1 * g
    v = 0.95 * v + 0.05 * g * g
    step = m * lax.rsqrt(v + 1e-8) + 0.1 * w
    return (w - 0.02 * step).astype(bf16), m, v


def clipped(gradients, sum_of_squares, count):
    factor = jnp.minimum(1.0, 0.5 * lax.rsqrt(sum_of_squares / count + 1e-30))
    return [g * factor for g in gradients]


def solution(mesh):
    def fetched(weights, number):
        return [lax.all_gather(w[number], "s", axis=0, tiled=True) for w in weights]

    def summed(term):
        return lax.psum(lax.psum_scatter(term, "s", scatter_dimension=0, tiled=True), "r")

    def step(x, dy, *arrays):
        weights, m, v = (arrays[i : i + 3] for i in (0, 3, 6))
        first, second = fetched(weights, 0), fetched(weights, 1)
        kept, h = forward(x[0], *first)
        *terms1, by_h = middle(h, dy[0], *second)
        terms0 = last(x[0], by_h, kept, first[2])
        mine = [[summed(t) for t in terms0], [summed(t) for t in terms1]]
        gradients = [jnp.stack([mine[number][i] for number in range(2)]).astype(f32) for i in range(3)]
        squares = lax.psum(sum(jnp.sum(g * g) for g in gradients), "s")
        gradients = clipped(gradients, squares, lax.psum(1, "s") * sum(g.size for g in gradients))
        new = [adamw(w.astype(f32), m, v, g) for w, m, v, g in zip(weights, m, v, gradients, strict=True)]
        return tuple(one[which] for which in range(3) for one in new)

    states, cut = P(("rep", "r", "s"), None, None), P(None, "s", None)
    return jax.shard_map(
        step,
        mesh=mesh,
        in_specs=(states, states) + (cut,) * 9,
        out_specs=(P("rep", "s", None),) * 9,
        check_vma=False,
    )
```

```python
import functools

import jax
import jax.numpy as jnp
from jax import lax
from jax.experimental import pallas as pl
from jax.experimental.pallas import tpu as pltpu
from jax.sharding import PartitionSpec as P

NAMES = ("w_gate", "w_up", "w_down")
bf16, f32 = jnp.bfloat16, jnp.float32
CH, SUB, TM, LANES = 256, 512, 1024, 128
NT_DIMS = (((1,), (1,)), ((), ()))
TN_DIMS = (((0,), (0,)), ((), ()))
VMEM_LIMIT = 67043328
MESH = pl.DeviceIdType.MESH


def groups_of(i):
    j, half = i // 2, i % 2
    first = j + 10 * half
    return first * LANES, (first + 5) * LANES


def dot(a, b):
    return jnp.dot(a, b, preferred_element_type=f32)


def rows_at(start, size, multiple=None):
    return pl.ds(pl.multiple_of(start, multiple or size), size)


def sigmoid(x):
    return 1.0 / (1.0 + jnp.exp(-x))


def columns_in(w_hbm, buf, sem, i, offset):
    return [
        pltpu.make_async_copy(w_hbm.at[:, rows_at(start, LANES)], buf.at[:, pl.ds(offset + LANES * n, LANES)], sem.at[n])
        for n, start in enumerate(groups_of(i))
    ]


def rows_in(w_hbm, buf, sem, i):
    return [
        pltpu.make_async_copy(w_hbm.at[rows_at(start, LANES), :], buf.at[pl.ds(LANES * n, LANES), :], sem.at[n])
        for n, start in enumerate(groups_of(i))
    ]


def start(copies):
    for c in copies:
        c.start()


def wait(copies):
    for c in copies:
        c.wait()


def normed_in_place(a_ref, aT_ref, t):
    rows = rows_at(t * 256, 256)
    w = a_ref[rows, :].astype(f32)
    a = (w * lax.rsqrt(jnp.mean(w * w, -1, keepdims=True) + 1e-6)).astype(bf16)
    a_ref[rows, :] = a
    if aT_ref is not None:
        aT_ref[:, rows] = a.T


def forward_kernel(h_hbm, wg_hbm, wu_hbm, wd_hbm, gu_hbm, out_hbm, a_ref, act_ref, wgu, wd, gus, hin, hout, hsem, wsem, wdsem, gsem, xsem, osem):
    T, D = a_ref.shape
    F = act_ref.shape[1]
    NC, NT = F // CH, T // TM

    def loads(t):
        rows = rows_at(t * 256, 256)
        return [pltpu.make_async_copy(h_hbm.at[rows, :], a_ref.at[rows, :], hsem.at[t])]

    def weights(i):
        slot = i % 2
        return columns_in(wg_hbm, wgu.at[slot], wsem.at[slot, 0], i, 0) + columns_in(wu_hbm, wgu.at[slot], wsem.at[slot, 1], i, CH)

    def saves(n):
        i, t = n // NT, n % NT
        return [pltpu.make_async_copy(gus.at[n % 2], gu_hbm.at[i, rows_at(t * TM, TM), :], gsem.at[n % 2])]

    def downs(i):
        return rows_in(wd_hbm, wd.at[rows_at(i * CH, CH), :], wdsem.at[i], i)

    lax.fori_loop(0, T // 256, lambda t, _: start(loads(t)) or 0, 0)
    start(weights(0))

    def norm(t, _):
        wait(loads(t))
        normed_in_place(a_ref, None, t)
        return 0

    lax.fori_loop(0, T // 256, norm, 0)
    lax.fori_loop(0, NC, lambda i, _: start(downs(i)) or 0, 0)

    def chunk(i, _):
        slot = i % 2
        wait(weights(i))

        @pl.when(i + 1 < NC)
        def _():
            start(weights(i + 1))

        def tile(t, _):
            n = i * NT + t

            @pl.when(n >= 2)
            def _():
                wait(saves(n - 2))

            def dots(k):
                gu = dot(a_ref[rows_at(t * TM + k * SUB, SUB), :], wgu[slot])
                gus[n % 2, pl.ds(k * SUB, SUB), :] = gu
                return gu

            def elementwise(k, gu):
                gate, up = gu[:, :CH], gu[:, CH:]
                act_ref[rows_at(t * TM + k * SUB, SUB), rows_at(i * CH, CH)] = (gate * sigmoid(gate) * up).astype(bf16)

            gu = dots(0)
            for k in range(TM // SUB):
                following = dots(k + 1) if k + 1 < TM // SUB else None
                elementwise(k, gu)
                gu = following
            start(saves(n))
            return 0

        lax.fori_loop(0, NT, tile, 0)
        return 0

    lax.fori_loop(0, NC, chunk, 0)
    lax.fori_loop(0, NC, lambda i, _: wait(downs(i)) or 0, 0)

    def inputs(t):
        return [pltpu.make_async_copy(h_hbm.at[rows_at(t * SUB, SUB), :], hin.at[t % 2], xsem.at[t % 2])]

    def outputs(t):
        return [pltpu.make_async_copy(hout.at[t % 2], out_hbm.at[rows_at(t * SUB, SUB), :], osem.at[t % 2])]

    start(inputs(0))

    def down(t, _):
        wait(inputs(t))

        @pl.when(t + 1 < T // SUB)
        def _():
            start(inputs(t + 1))

        @pl.when(t >= 2)
        def _():
            wait(outputs(t - 2))

        out = dot(act_ref[rows_at(t * SUB, SUB), :], wd[...]).astype(bf16)
        hout[t % 2] = (hin[t % 2].astype(f32) + out.astype(f32)).astype(bf16)
        start(outputs(t))
        return 0

    lax.fori_loop(0, T // SUB, down, 0)
    for n in (NC * NT - 2, NC * NT - 1):
        wait(saves(n))
    for t in (T // SUB - 2, T // SUB - 1):
        wait(outputs(t))


def when(condition):
    if isinstance(condition, bool):
        return (lambda f: f()) if condition else (lambda f: None)
    return pl.when(condition)


class Place:
    def __init__(self):
        s = lax.axis_index("s")
        self.c, self.y, self.x = s % 2, (s // 2) % 2, s // 4
        self.core = {"s": s + 1 - 2 * self.c}
        self.over_y = {"s": s + 2 - 4 * self.y}
        self.over_x = {"s": s + 4 - 8 * self.x}
        self.over_z = {"r": 1 - lax.axis_index("r")}

    def barrier(self):
        barrier = pltpu.get_barrier_semaphore()
        for device in (self.core, self.over_y, self.over_x, self.over_z):
            pl.semaphore_signal(barrier, inc=1, device_id=device, device_id_type=MESH)
        pl.semaphore_wait(barrier, 4)


def remote(source, target, send, receive, device):
    return pltpu.make_async_remote_copy(source, target, send, receive, device_id=device, device_id_type=MESH)


def give(semaphore, device):
    pl.semaphore_signal(semaphore, inc=1, device_id=device, device_id_type=MESH)


class Reducer:
    SHAPES = (((2, 4, 2), bf16), ((4, 2), bf16), ((2, 2), bf16), ((2, 2), f32), ((2, 2), bf16), ((2,), bf16), ((2,), f32), ((2,), bf16), ((2,), bf16), ((2,), bf16), ((2,), bf16))

    @classmethod
    def scratch(cls, slots, block):
        D, R = pltpu.SemaphoreType.DMA, pltpu.SemaphoreType.REGULAR
        buffers = [pltpu.VMEM((slots,) + lead + block, kind) for lead, kind in cls.SHAPES]
        return buffers + [D((2, slots)), D((2, slots, 2)), D((2, slots, 2)), D((2, slots)), R((slots,)), R((slots, 2)), R((slots, 2)), R((slots,)), pltpu.VMEM((8, block[1]), f32)]

    COUNT = 20

    def __init__(self, place, refs):
        self.place = place
        self.all, self.got0, self.out1, self.kept1, self.got1, self.out2, self.kept2, self.got2, self.out3, self.got3, self.out = refs[:11]
        self.sem0, self.sem1, self.sem2, self.sem3, self.free0, self.free1, self.free2, self.free3, self.squares = refs[11:]
        self.squares[...] = jnp.zeros_like(self.squares)
        self.first_way, self.second_way = (place.over_x, place.over_y), (place.over_y, place.over_x)

    def copy0(self, b):
        return remote(self.all.at[b, 1 - self.place.c], self.got0.at[b], self.sem0.at[0, b], self.sem0.at[1, b], self.place.core)

    def copy1(self, b, p):
        return remote(self.out1.at[b, p], self.got1.at[b, p], self.sem1.at[0, b, p], self.sem1.at[1, b, p], self.first_way[p])

    def copy2(self, b, p):
        return remote(self.out2.at[b, p], self.got2.at[b, p], self.sem2.at[0, b, p], self.sem2.at[1, b, p], self.second_way[p])

    def copy3(self, b):
        return remote(self.out3.at[b], self.got3.at[b], self.sem3.at[0, b], self.sem3.at[1, b], self.place.over_z)

    def send(self, b, first):
        @when(not first if isinstance(first, bool) else jnp.logical_not(first))
        def _():
            pl.semaphore_wait(self.free0.at[b], 1)

        self.copy0(b).start()

    def after_core(self, b, first, final):
        place, c = self.place, self.place.c
        self.copy0(b).wait()
        for p in range(2):
            for n in range(2):
                away, near = ((1 - place.x) * 2 + n, place.x * 2 + n) if p == 0 else (n * 2 + 1 - place.y, n * 2 + place.y)
                self.out1[b, p, n] = (self.all[b, c, away, p].astype(f32) + self.got0[b, away, p].astype(f32)).astype(bf16)
                self.kept1[b, p, n] = self.all[b, c, near, p].astype(f32) + self.got0[b, near, p].astype(f32)

        @when(not final if isinstance(final, bool) else jnp.logical_not(final))
        def _():
            give(self.free0.at[b], place.core)

        @when(not first if isinstance(first, bool) else jnp.logical_not(first))
        def _():
            for p in range(2):
                pl.semaphore_wait(self.free1.at[b, p], 1)

        for p in range(2):
            self.copy1(b, p).start()

    def after_first(self, b, first, final):
        place = self.place
        for p in range(2):
            self.copy1(b, p).wait()
            near = place.y if p == 0 else place.x
            self.out2[b, p] = (self.kept1[b, p, 1 - near] + self.got1[b, p, 1 - near].astype(f32)).astype(bf16)
            self.kept2[b, p] = self.kept1[b, p, near] + self.got1[b, p, near].astype(f32)

        @when(not final if isinstance(final, bool) else jnp.logical_not(final))
        def _():
            for p in range(2):
                give(self.free1.at[b, p], self.first_way[p])

        @when(not first if isinstance(first, bool) else jnp.logical_not(first))
        def _():
            for p in range(2):
                pl.semaphore_wait(self.free2.at[b, p], 1)

        for p in range(2):
            self.copy2(b, p).start()

    def after_second(self, b, first, final):
        for p in range(2):
            self.copy2(b, p).wait()
            self.out3[b, p] = (self.kept2[b, p] + self.got2[b, p].astype(f32)).astype(bf16)

        @when(not final if isinstance(final, bool) else jnp.logical_not(final))
        def _():
            for p in range(2):
                give(self.free2.at[b, p], self.second_way[p])

        @when(not first if isinstance(first, bool) else jnp.logical_not(first))
        def _():
            pl.semaphore_wait(self.free3.at[b], 1)

        self.copy3(b).start()

    def after_copy(self, b, final):
        self.copy3(b).wait()
        for p in range(2):
            g = (self.out3[b, p].astype(f32) + self.got3[b, p].astype(f32)).astype(bf16)
            self.out[b, p] = g
            g = g.astype(f32)
            self.squares[...] += jnp.sum((g * g).reshape(g.shape[0] // 8, 8, g.shape[1]), 0)

        @when(not final if isinstance(final, bool) else jnp.logical_not(final))
        def _():
            give(self.free3.at[b], self.place.over_z)


class Gradients:
    @staticmethod
    def scratch(rows, down_rows, D):
        V, S = pltpu.VMEM, pltpu.SemaphoreType.DMA
        return (
            Reducer.scratch(2, (rows, CH)) + Reducer.scratch(1, (32, D))
            + [V((5, 64, D), bf16), S((2, 2, 2)), S((5,)), S((2, 2))]
        )

    def __init__(self, place, refs, outs, NC):
        n = Reducer.COUNT
        self.place, self.NC = place, NC
        self.wide = Reducer(place, refs[:n])
        self.down = Reducer(place, refs[n : 2 * n])
        self.down_out, self.out_sem, self.local_sem, self.cross_sem = refs[2 * n :]
        self.gate_hbm, self.up_hbm, self.down_hbm = outs

    def flags(self, i):
        b = i % 2
        return b, i < 2, i + 2 >= self.NC

    def put_wide(self, i, value):
        b, rows = i % 2, value.shape[0] // 8
        value = value.astype(bf16)
        for s in range(8):
            for p in range(2):
                self.wide.all[b, s % 2, s // 2, p] = value[rows * s : rows * (s + 1), CH * p : CH * (p + 1)]

    def put_down(self, i, value):
        half = i % 2
        value = value.astype(bf16)
        for n in range(2):
            for core in range(2):
                for p in range(2):
                    at = LANES * n + 64 * core + 32 * p
                    self.down.all[0, core, 2 * half + n, p] = value[at : at + 32]

    def wide_send(self, i):
        b, first, _ = self.flags(i)
        self.wide.send(b, first)

    def wide1(self, i):
        self.wide.after_core(*self.flags(i))

    def wide2(self, i):
        self.wide.after_first(*self.flags(i))

    def wide3(self, i):
        self.wide.after_second(*self.flags(i))

    def wide_outs(self, i):
        b = i % 2
        return [
            pltpu.make_async_copy(
                self.wide.out.at[b, p, :, pl.ds(LANES * n, LANES)], (self.gate_hbm, self.up_hbm)[p].at[:, rows_at(at, LANES)], self.out_sem.at[b, p, n]
            )
            for p in range(2)
            for n, at in enumerate(groups_of(i))
        ]

    def wide4(self, i):
        b, first, final = self.flags(i)

        @when(not first if isinstance(first, bool) else jnp.logical_not(first))
        def _():
            wait(self.wide_outs(i - 2))

        self.wide.after_copy(b, final)
        start(self.wide_outs(i))

    def rounds(self, j):
        return 0, j < 1, j >= self.NC // 2 - 1

    def down_send(self, j):
        self.down.send(0, j < 1)

    def down1(self, j):
        self.down.after_core(*self.rounds(j))

    def down2(self, j):
        self.down.after_first(*self.rounds(j))

    def down3(self, j):
        self.down.after_second(*self.rounds(j))

    def down_rows(self, j):
        unit = 2 * j + self.place.c
        return rows_at((unit % 5) * 64, 64), unit // 5 == self.place.c

    def down_local(self, j):
        rows, _ = self.down_rows(j)
        return pltpu.make_async_copy(self.down_out.at[j], self.down_hbm.at[rows, :], self.local_sem.at[j])

    def down_cross(self, j):
        rows, _ = self.down_rows(j)
        return remote(self.down_out.at[j], self.down_hbm.at[rows, :], self.cross_sem.at[0, j % 3], self.cross_sem.at[1, j % 3], self.place.core)

    def down4(self, j):
        self.down.after_copy(0, self.rounds(j)[2])
        for p in range(2):
            self.down_out[j, pl.ds(32 * p, 32), :] = self.down.out[0, p]
        _, mine = self.down_rows(j)

        @pl.when(mine)
        def _():
            self.down_local(j).start()

        @pl.when(jnp.logical_not(mine))
        def _():
            self.down_cross(j).start()

    def in_tiles(self, i):
        @when(i >= 1)
        def _():
            self.wide1(i - 1)

        @when(i >= 3)
        def _():
            self.wide4(i - 3)

    def after_down(self, i):
        j = i // 2

        @when(i % 2 == 1)
        def _():
            @when(i >= 3)
            def _():
                self.down4(j - 1)

            self.down_send(j)

        @when(jnp.logical_and(i % 2 == 0, i >= 2))
        def _():
            self.down2(j - 1)

        @when(i >= 2)
        def _():
            self.wide3(i - 2)

    def after_wide(self, i):
        j = i // 2
        self.wide_send(i)

        @when(i >= 1)
        def _():
            self.wide2(i - 1)

        @when(i % 2 == 1)
        def _():
            self.down1(j)

        @when(jnp.logical_and(i % 2 == 0, i >= 2))
        def _():
            self.down3(j - 1)

    def tail(self):
        n, j = self.NC, self.NC // 2 - 1

        def first():
            self.wide4(n - 3)
            self.wide3(n - 2)
            self.down2(j)
            self.wide1(n - 1)

        def second():
            self.down3(j)
            self.wide4(n - 2)
            self.wide2(n - 1)

        def third():
            self.down4(j)
            self.wide3(n - 1)

        def fourth():
            self.wide4(n - 1)

        return first, second, third, fourth

    def squares(self):
        total = jnp.zeros((8, LANES), f32)
        for ref in (self.wide.squares, self.down.squares):
            for n in range(ref.shape[1] // LANES):
                total += ref[:, pl.ds(LANES * n, LANES)]
        return total

    def finish(self):
        for i in (self.NC - 2, self.NC - 1):
            wait(self.wide_outs(i))
        for j in range(5):
            _, mine = self.down_rows(j)

            @pl.when(mine)
            def _():
                self.down_local(j).wait()

            @pl.when(jnp.logical_not(mine))
            def _():
                self.down_cross(j).wait_send()

        for n in range(2):
            self.down_cross(n).wait_recv()


def middle_kernel(h_hbm, dy_hbm, wg_hbm, wu_hbm, wd_hbm, gg_hbm, gu_hbm, gd_hbm, dh_hbm, sq_hbm,
                  a_ref, aT_ref, dy_ref, da_ref, dgu_ref, act_ref, wgu, wd, sq, hsem, ysem, wsem, qsem, *refs):
    T, D = a_ref.shape
    F = wg_hbm.shape[1]
    NC, NT = F // CH, T // TM

    def loads(t):
        rows = rows_at(t * 256, 256)
        return [pltpu.make_async_copy(h_hbm.at[rows, :], a_ref.at[rows, :], hsem.at[t])]

    def dys():
        return [pltpu.make_async_copy(dy_hbm, dy_ref, ysem)]

    def weights(i):
        slot = i % 2
        return (
            columns_in(wg_hbm, wgu.at[slot], wsem.at[slot, 0], i, 0)
            + columns_in(wu_hbm, wgu.at[slot], wsem.at[slot, 1], i, CH)
            + rows_in(wd_hbm, wd.at[slot], wsem.at[slot, 2], i)
        )

    lax.fori_loop(0, T // 256, lambda t, _: start(loads(t)) or 0, 0)
    start(weights(0))
    start(dys())
    place = Place()
    gradients = Gradients(place, refs, (gg_hbm, gu_hbm, gd_hbm), NC)
    place.barrier()

    def norm(t, _):
        wait(loads(t))
        normed_in_place(a_ref, aT_ref, t)
        da_ref[rows_at(t * 256, 256), :] = jnp.zeros((256, D), f32)
        return 0

    lax.fori_loop(0, T // 256, norm, 0)
    wait(dys())

    def chunk(i, _):
        slot = i % 2
        wait(weights(i))

        @pl.when(i + 1 < NC)
        def _():
            start(weights(i + 1))

        def tile(t, _):
            @pl.when(t == 2)
            def _():
                gradients.in_tiles(i)

            def rows_of(k):
                return rows_at(t * TM + k * SUB, SUB)

            def dots(k):
                rows = rows_of(k)
                return dot(a_ref[rows, :], wgu[slot]), lax.dot_general(dy_ref[rows, :], wd[slot], NT_DIMS, preferred_element_type=f32)

            def elementwise(k, gu, dact):
                rows = rows_of(k)
                dact = dact.astype(bf16).astype(f32)
                gate, up = gu[:, :CH], gu[:, CH:]
                sg = sigmoid(gate)
                silu = gate * sg
                act_ref[rows, :] = (silu * up).astype(bf16)
                dgate = (dact * up * (sg * (1.0 + gate * (1.0 - sg)))).astype(bf16)
                dup = (dact * silu).astype(bf16)
                dgu_ref[rows, pl.ds(0, CH)] = dgate
                dgu_ref[rows, pl.ds(CH, CH)] = dup
                return jnp.concatenate([dgate, dup], 1)

            def back(k, dgu):
                da_ref[rows_of(k), :] += lax.dot_general(dgu, wgu[slot], NT_DIMS, preferred_element_type=f32)

            now, before = dots(0), None
            for k in range(TM // SUB):
                following = dots(k + 1) if k + 1 < TM // SUB else None
                dgu = elementwise(k, *now)
                if before is not None:
                    back(k - 1, before)
                before, now = dgu, following
            back(TM // SUB - 1, before)
            return 0

        lax.fori_loop(0, NT, tile, 0)

        gradients.put_down(i, lax.dot_general(act_ref[...], dy_ref[...], TN_DIMS, preferred_element_type=f32))
        gradients.after_down(i)
        gradients.put_wide(i, dot(aT_ref[...], dgu_ref[...]))
        gradients.after_wide(i)
        return 0

    lax.fori_loop(0, NC, chunk, 0)
    lax.fori_loop(0, T // 256, lambda t, _: start(loads(t)) or 0, 0)

    def stores(t):
        rows = rows_at(t * 256, 256)
        return [pltpu.make_async_copy(dy_ref.at[rows, :], dh_hbm.at[rows, :], hsem.at[t])]

    def norm_back(t, _):
        rows = rows_at(t * 256, 256)
        wait(loads(t))
        w = a_ref[rows, :].astype(f32)
        da = da_ref[rows, :].astype(bf16).astype(f32)
        scale = lax.rsqrt(jnp.mean(w * w, -1, keepdims=True) + 1e-6)
        along = jnp.sum(da * w, -1, keepdims=True) * (scale * scale * scale) * (1.0 / D)
        by_h = (da * scale - w * along).astype(bf16)
        dy_ref[rows, :] = (dy_ref[rows, :].astype(f32) + by_h.astype(f32)).astype(bf16)
        start(stores(t))
        for at, step in ((T // 512 - 2, second), (T // 256 - 5, third)):
            pl.when(t == at)(step)
        return 0

    first, second, third, fourth = gradients.tail()
    first()
    lax.fori_loop(0, T // 256, norm_back, 0)
    fourth()
    sq[...] = gradients.squares()
    done = pltpu.make_async_copy(sq, sq_hbm, qsem)
    done.start()
    lax.fori_loop(0, T // 256, lambda t, _: wait(stores(t)) or 0, 0)
    gradients.finish()
    done.wait()


def last_kernel(h_hbm, dy_hbm, kept_hbm, wd_hbm, sq_in, gg_hbm, gu_hbm, gd_hbm, sq_hbm,
                a_ref, aT_ref, dy_ref, dgu_ref, act_ref, gus, wd, sq, parts, hsem, ysem, gsem, wsem, qsem, psem, *refs):
    T, D = a_ref.shape
    F = wd_hbm.shape[0]
    NC, NT = F // CH, T // TM

    def loads(t):
        rows = rows_at(t * 256, 256)
        return [pltpu.make_async_copy(h_hbm.at[rows, :], a_ref.at[rows, :], hsem.at[t])]

    def dys():
        return [pltpu.make_async_copy(dy_hbm, dy_ref, ysem)]

    def weights(i):
        slot = i % 2
        return rows_in(wd_hbm, wd.at[slot], wsem.at[slot], i)

    def kept(n):
        i, t = n // NT, n % NT
        return [pltpu.make_async_copy(kept_hbm.at[i, rows_at(t * TM, TM), :], gus.at[n % NT], gsem.at[n % NT])]

    lax.fori_loop(0, T // 256, lambda t, _: start(loads(t)) or 0, 0)
    start(weights(0))
    start(dys())
    for n in range(NT):
        start(kept(n))
    before = pltpu.make_async_copy(sq_in, sq, qsem)
    before.start()
    place = Place()
    gradients = Gradients(place, refs, (gg_hbm, gu_hbm, gd_hbm), NC)
    place.barrier()

    def norm(t, _):
        wait(loads(t))
        normed_in_place(a_ref, aT_ref, t)
        return 0

    lax.fori_loop(0, T // 256, norm, 0)
    wait(dys())

    def chunk(i, _):
        slot = i % 2
        wait(weights(i))

        @pl.when(i + 1 < NC)
        def _():
            start(weights(i + 1))

        def tile(t, _):
            n = i * NT + t
            wait(kept(n))

            @pl.when(t == 2)
            def _():
                gradients.in_tiles(i)

            def rows_of(k):
                return rows_at(t * TM + k * SUB, SUB)

            def dots(k):
                return lax.dot_general(dy_ref[rows_of(k), :], wd[slot], NT_DIMS, preferred_element_type=f32)

            def elementwise(k, dact):
                rows = rows_of(k)
                dact = dact.astype(bf16).astype(f32)
                gate, up = gus[t, pl.ds(k * SUB, SUB), pl.ds(0, CH)], gus[t, pl.ds(k * SUB, SUB), pl.ds(CH, CH)]
                sg = sigmoid(gate)
                silu = gate * sg
                act_ref[rows, :] = (silu * up).astype(bf16)
                dgu_ref[rows, pl.ds(0, CH)] = (dact * up * (sg * (1.0 + gate * (1.0 - sg)))).astype(bf16)
                dgu_ref[rows, pl.ds(CH, CH)] = (dact * silu).astype(bf16)

            now = dots(0)
            for k in range(TM // SUB):
                following = dots(k + 1) if k + 1 < TM // SUB else None
                elementwise(k, now)
                now = following

            @pl.when(n + NT < NC * NT)
            def _():
                start(kept(n + NT))

            return 0

        lax.fori_loop(0, NT, tile, 0)

        gradients.put_down(i, lax.dot_general(act_ref[...], dy_ref[...], TN_DIMS, preferred_element_type=f32))
        gradients.after_down(i)
        gradients.put_wide(i, dot(aT_ref[...], dgu_ref[...]))
        gradients.after_wide(i)
        return 0

    lax.fori_loop(0, NC, chunk, 0)
    before.wait()
    for step in gradients.tail():
        step()
    sq[...] += gradients.squares()
    for n, device in enumerate((place.core, place.over_y, place.over_x)):
        parts[0, n] = sq[...]
        exchange = remote(parts.at[0, n], parts.at[1, n], psem.at[0, n], psem.at[1, n], device)
        exchange.start()
        exchange.wait()
        sq[...] += parts[1, n]
    done = pltpu.make_async_copy(sq, sq_hbm, qsem)
    done.start()
    gradients.finish()
    done.wait()


def call(kernel, outs, scratch, inputs, **params):
    anywhere = pl.BlockSpec(memory_space=pl.ANY)
    return pl.pallas_call(
        kernel,
        out_shape=[jax.ShapeDtypeStruct(*o) for o in outs],
        in_specs=[anywhere] * len(inputs),
        out_specs=[anywhere] * len(outs),
        scratch_shapes=scratch,
        compiler_params=pltpu.CompilerParams(vmem_limit_bytes=VMEM_LIMIT, **params),
    )(*inputs)


def forward(h, wg, wu, wd):
    (T, D), F = h.shape, wg.shape[1]
    V, S = pltpu.VMEM, pltpu.SemaphoreType.DMA
    return call(
        forward_kernel,
        [((F // CH, T, 2 * CH), f32), ((T, D), bf16)],
        [V((T, D), bf16), V((T, F), bf16), V((2, D, 2 * CH), bf16), V((F, D), bf16), V((2, TM, 2 * CH), f32), V((2, SUB, D), bf16), V((2, SUB, D), bf16)]
        + [S((T // 256,)), S((2, 2, 2)), S((F // CH, 2)), S((2,)), S((2,)), S((2,))],
        (h, wg, wu, wd),
    )


def middle(h, dy, wg, wu, wd):
    (T, D), F = h.shape, wg.shape[1]
    V, S = pltpu.VMEM, pltpu.SemaphoreType.DMA
    return call(
        middle_kernel,
        [((D // 8, F), bf16), ((D // 8, F), bf16), ((F // 8, D), bf16), ((T, D), bf16), ((8, LANES), f32)],
        [V((T, D), bf16), V((D, T), bf16), V((T, D), bf16), V((T, D), f32), V((T, 2 * CH), bf16), V((T, CH), bf16)]
        + [V((2, D, 2 * CH), bf16), V((2, CH, D), bf16), V((8, LANES), f32)]
        + [S((T // 256,)), S(()), S((2, 3, 2)), S(())]
        + Gradients.scratch(D // 8, F // 8, D),
        (h, dy, wg, wu, wd),
        collective_id=1,
        has_side_effects=True,
    )


def last(h, dy, gu, wd, squares):
    (T, D), F = h.shape, wd.shape[0]
    V, S = pltpu.VMEM, pltpu.SemaphoreType.DMA
    return call(
        last_kernel,
        [((D // 8, F), bf16), ((D // 8, F), bf16), ((F // 8, D), bf16), ((8, LANES), f32)],
        [V((T, D), bf16), V((D, T), bf16), V((T, D), bf16), V((T, 2 * CH), bf16), V((T, CH), bf16), V((T // TM, TM, 2 * CH), f32)]
        + [V((2, CH, D), bf16), V((8, LANES), f32), V((2, 3, 8, LANES), f32)]
        + [S((T // 256,)), S(()), S((T // TM,)), S((2, 2)), S(()), S((2, 3))]
        + Gradients.scratch(D // 8, F // 8, D),
        (h, dy, gu, wd, squares),
        collective_id=2,
        has_side_effects=True,
    )


def adamw(w, m, v, g):
    m = 0.9 * m + 0.1 * g
    v = 0.95 * v + 0.05 * g * g
    step = m * lax.rsqrt(v + 1e-8) + 0.1 * w
    return (w - 0.02 * step).astype(bf16), m, v


def clipped(gradients, sum_of_squares, count):
    factor = jnp.minimum(1.0, 0.5 * lax.rsqrt(sum_of_squares / count + 1e-30))
    return [g * factor for g in gradients]


def solution(mesh):
    def fetched(weights, number):
        return [lax.all_gather(w[number], "s", axis=0, tiled=True) for w in weights]

    def step(x, dy, *arrays):
        weights, m, v = (arrays[i : i + 3] for i in (0, 3, 6))
        first, second = fetched(weights, 0), fetched(weights, 1)
        kept, h = forward(x[0], *first)
        *second_sums, by_h, squares = middle(h, dy[0], *second)
        *first_sums, squares = last(x[0], by_h, kept, first[2], squares)
        gradients = [jnp.stack(pair).astype(f32) for pair in zip(first_sums, second_sums, strict=True)]
        gradients = clipped(gradients, jnp.sum(squares), lax.psum(1, "s") * sum(g.size for g in gradients))
        new = [adamw(w.astype(f32), m, v, g) for w, m, v, g in zip(weights, m, v, gradients, strict=True)]
        return tuple(one[which] for which in range(3) for one in new)

    states, cut = P(("rep", "r", "s"), None, None), P(None, "s", None)
    return jax.shard_map(
        step,
        mesh=mesh,
        in_specs=(states, states) + (cut,) * 9,
        out_specs=(P("rep", "s", None),) * 9,
        check_vma=False,
    )
```

```python
import functools
import re

import jax
import jax.numpy as jnp
from jax import lax
from jax.experimental import pallas as pl
from jax.experimental.pallas import tpu as pltpu
from jax.sharding import PartitionSpec as P

bf16, f32 = jnp.bfloat16, jnp.float32
CH, SUB, TM, LANES, ROWS, UNIT = 256, 512, 1024, 128, 256, 64
HALF, BOTH = UNIT // 2, 2 * CH
SMALL, TWO, TWO_THREE = (8, LANES), (2,), (2, 3)
PAIR = range(2)
NT_DIMS = (((1,), (1,)), ((), ()))
TN_DIMS = (((0,), (0,)), ((), ()))
VMEM_LIMIT = 67043328
MESH = pl.DeviceIdType.MESH
EPS = 1e-6
LAST_CHUNK, LAST_ROUND = 9, 4
ANY = pl.BlockSpec(memory_space=pl.ANY)
V, DMA, REGULAR = pltpu.VMEM, pltpu.SemaphoreType.DMA, pltpu.SemaphoreType.REGULAR
local = pltpu.make_async_copy


NORM_PLAN = "s0s1//s2/"
TILE_PLAN = "".join((
    "f0x0c0f1f2s3/s4/x1c1x2s5/c2f3s6/f4/",
    "x3f5s7/c3f6x4s8/c4x5s9/c5x6f7/c6f8s10/",
    "f9/x7x8/c7c8s11/x9f10/c9s12/",
    "f11/x10s13/c10f12/x11/c11s14/",
))
DOWN_PLAN = "x12c12f13//f14/x13/c13x14/c14//"
END_PLAN = ""


def odd(i):
    return i % 2


def groups_of(i):
    first = i // 2 + 10 * odd(i)
    return first * LANES, (first + 5) * LANES


def dot(a, b):
    return jnp.dot(a, b, preferred_element_type=f32)


def dot_nt(a, b):
    return lax.dot_general(a, b, NT_DIMS, preferred_element_type=f32)


def dot_tn(a, b):
    return lax.dot_general(a, b, TN_DIMS, preferred_element_type=f32)


def at(start, size, multiple=None):
    return pl.ds(pl.multiple_of(start, multiple or size), size)


def block(t, size):
    return at(t * size, size)


def wide(x):
    return x.astype(f32)


def sigmoid(x):
    return 1.0 / (1.0 + jnp.exp(-x))


def start(*copies):
    for c in copies:
        c.start()


def wait(*copies):
    for c in copies:
        c.wait()


def loop(count, body, first=0):
    def turn(t, carry):
        body(t)
        return carry

    lax.fori_loop(first, count, turn, 0)


def when(condition):
    if isinstance(condition, bool):
        return (lambda f: f()) if condition else (lambda f: None)
    return pl.when(condition)


def unless(condition):
    return when(not condition if isinstance(condition, bool) else jnp.logical_not(condition))


def branch(condition):
    if isinstance(condition, bool):
        return when(condition)
    return lambda f: loop(condition.astype(jnp.int32), lambda _: f())


def both(a, b):
    return a and b if isinstance(a, bool) and isinstance(b, bool) else jnp.logical_and(a, b)


def rows_in(w_hbm, buf, sem, i):
    return [local(w_hbm.at[at(s, LANES), :], buf.at[block(n, LANES), :], sem.at[n]) for n, s in enumerate(groups_of(i))]


def norm_scale(w):
    return lax.rsqrt(jnp.mean(w * w, -1, keepdims=True) + EPS)


def normed(w):
    return (w * norm_scale(w)).astype(bf16)


class Place:
    def __init__(self):
        self.s = s = lax.axis_index("s")
        self.c, self.y, self.x = odd(s), odd(s // 2), s // 4
        other, across_x, across_y = 1 - 2 * self.c, 4 - 8 * self.x, 2 - 4 * self.y
        self.core, self.over_x, self.over_y = {"s": s + other}, {"s": s + across_x}, {"s": s + across_y}
        self.over_z = {"r": 1 - lax.axis_index("r")}
        self.mine = (s, s + across_x, s + across_y, s + across_x + across_y)
        self.others = tuple(o + other for o in self.mine)
        self.peers = self.mine[1:] + self.others

    def barrier(self, across=True, all_peers=False):
        barrier = pltpu.get_barrier_semaphore()
        neighbours = [{"s": s} for s in self.peers] if all_peers else [self.core, self.over_y, self.over_x]
        if across:
            neighbours.append(self.over_z)
        for device in neighbours:
            give(barrier, device)
        pl.semaphore_wait(barrier, len(neighbours))


def remote(source, target, send, receive, device):
    return pltpu.make_async_remote_copy(source, target, send, receive, device_id=device, device_id_type=MESH)


def give(semaphore, device):
    pl.semaphore_signal(semaphore, inc=1, device_id=device, device_id_type=MESH)


def take(semaphore):
    pl.semaphore_wait(semaphore, 1)


class Reducer:
    SHAPES = ("ocp", "cp", "pp", "pp", "p", "p", "p", "p", "p")

    @classmethod
    def scratch(cls, shape):
        sizes = {"o": (2, 4), "c": (4,), "p": (2,)}
        buffers = [V((2,) + sum((sizes[c] for c in lead if c != "c" or "o" not in lead), ()) + shape, bf16) for lead in cls.SHAPES]
        one, two = (2,), (2, 2)
        return buffers + [DMA((2,) + n) for n in (one, two, two, one)] + [REGULAR(n) for n in (one, two, two, one)] + [V((8, shape[1]), f32)]

    COUNT = 18

    def __init__(self, place, refs):
        self.place = place
        self.all, self.got0, self.out1, self.got1, self.out2, self.got2, self.out3, self.got3, self.out = refs[:9]
        self.sem0, self.sem1, self.sem2, self.sem3, self.free0, self.free1, self.free2, self.free3, self.squares = refs[9:]
        self.squares[...] = jnp.zeros_like(self.squares)
        self.first_way, self.second_way = (place.over_x, place.over_y), (place.over_y, place.over_x)

    def copy0(self, b):
        return remote(self.all.at[b, 1 - self.place.c], self.got0.at[b], self.sem0.at[0, b], self.sem0.at[1, b], self.place.core)

    def copy1(self, b, p):
        return remote(self.out1.at[b, p], self.got1.at[b, p], self.sem1.at[0, b, p], self.sem1.at[1, b, p], self.first_way[p])

    def copy2(self, b, p):
        return remote(self.out2.at[b, p], self.got2.at[b, p], self.sem2.at[0, b, p], self.sem2.at[1, b, p], self.second_way[p])

    def copy3(self, b):
        return remote(self.out3.at[b], self.got3.at[b], self.sem3.at[0, b], self.sem3.at[1, b], self.place.over_z)

    def chip_sum(self, b, p, x, y):
        k = 2 * x + y
        return wide(self.all[b, self.place.c, k, p]) + wide(self.got0[b, k, p])

    def send(self, b, first, final):
        unless(first)(lambda: take(self.free0.at[b]))
        self.copy0(b).start()

    def after_core(self, b, first, final):
        place = self.place
        self.copy0(b).wait()
        for p in PAIR:
            unless(first)(lambda: take(self.free1.at[b, p]))
            for n in PAIR:
                self.out1[b, p, n] = self.chip_sum(b, p, *((n, 1 - place.y) if p else (1 - place.x, n))).astype(bf16)
            self.copy1(b, p).start()

    def after_first(self, b, first, final):
        place = self.place
        for p in PAIR:
            self.copy1(b, p).wait()
            unless(first)(lambda: take(self.free2.at[b, p]))
            away = (1 - place.x, place.y) if p else (place.x, 1 - place.y)
            self.out2[b, p] = (self.chip_sum(b, p, *away) + wide(self.got1[b, p, away[1 - p]])).astype(bf16)
            self.copy2(b, p).start()

    def after_second(self, b, first, final):
        place = self.place
        for p in PAIR:
            self.copy2(b, p).wait()
            near = place.x if p else place.y
            self.out3[b, p] = (self.chip_sum(b, p, place.x, place.y) + wide(self.got1[b, p, near]) + wide(self.got2[b, p])).astype(bf16)
        unless(first)(lambda: take(self.free3.at[b]))
        self.copy3(b).start()

        def release():
            give(self.free0.at[b], place.core)
            for p in PAIR:
                give(self.free1.at[b, p], self.first_way[p])
                give(self.free2.at[b, p], self.second_way[p])

        unless(final)(release)

    def after_copy(self, b, first, final):
        self.copy3(b).wait()
        for p in PAIR:
            g = (wide(self.out3[b, p]) + wide(self.got3[b, p])).astype(bf16)
            self.out[b, p] = g
            g = wide(g)
            self.squares[...] += jnp.sum((g * g).reshape(-1, 8, g.shape[1]), 0)
        unless(final)(lambda: give(self.free3.at[b], self.place.over_z))


class Steps:
    def __init__(self, weights, layer, land, me, span=1, stage=None, first=0):
        self.weights, self.layer, self.land, self.me, self.span, self.stage, self.first = weights, layer, land, me, span, stage, first

    def own(self, q):
        return self.region(q, self.me) if self.stage is None else self.staged(q)


class WideSteps(Steps):
    @property
    def rows(self):
        return self.weights[0].shape[1]

    def region(self, q, owner):
        return self.land.at[pl.ds(q, self.span), at(self.rows * owner, self.rows, 16), :]

    def part(self, q, owner, p):
        return self.land.at[pl.ds(q, self.span), at(self.rows * owner, self.rows, 16), block(p, CH)]

    def staged(self, q):
        return self.stage.at[pl.ds(q - self.first, self.span)]

    def fetch(self, q, sem):
        for k in range(self.span):
            for p in PAIR:
                for n, s in enumerate(groups_of(q + k)):
                    lanes = at(CH * p + LANES * n, LANES)
                    if self.stage is None:
                        target = self.land.at[q + k, at(self.rows * self.me, self.rows, 16), lanes]
                    else:
                        target = self.stage.at[q + k - self.first, :, lanes]
                    local(self.weights[p].at[self.layer, :, at(s, LANES)], target, sem).start()


class DownSteps(Steps):
    @property
    def rows(self):
        return self.weights.shape[1]

    def region(self, q, owner):
        return self.land.at[at(self.rows * owner + UNIT * q, UNIT * self.span, UNIT), :]

    def part(self, q, owner, p):
        return self.land.at[at(self.rows * owner + UNIT * q + HALF * self.span * p, HALF * self.span, HALF), :]

    def staged(self, q):
        return self.stage.at[at(UNIT * (q - self.first), UNIT * self.span, UNIT), :]

    def fetch(self, q, sem):
        local(self.weights.at[self.layer, at(UNIT * q, UNIT * self.span, UNIT), :], self.own(q), sem).start()


class Gatherer:
    @staticmethod
    def scratch(steps):
        return [DMA((steps, 8)), DMA((2, 8)), DMA((steps,)), DMA((steps,))]

    COUNT = 4

    def __init__(self, place, steps, refs):
        self.place, self.steps = place, steps
        self.received, self.sent, self.fetched, self.homed = refs

    def each(self, m, f):
        for k, (kind, q) in enumerate(self.steps):
            branch(m == k)(functools.partial(f, kind, q, k))

    def copy(self, m, n, source, target, device):
        return remote(source, target, self.sent.at[odd(m), n], self.received.at[m, n], device)

    def push(self, m, n, region, device, source=None):
        copy = self.copy(m, n, region if source is None else source, region, device)
        if m >= 2:
            self.gone(m - 2, n)
        copy.start()

    def gone(self, m, n):
        kind, q = self.steps[m]
        region = kind.part(q, self.place.s, 0) if n in (4, 6) else kind.region(q, self.place.s)
        self.copy(m, n, region, region, self.place.core).wait_send()

    def landed(self, m, n, target):
        self.copy(m, n, target, target, self.place.core).wait_recv()

    def home(self, kind, q, m):
        return local(kind.own(q), kind.region(q, kind.me), self.homed.at[m])

    def fetch_all(self):
        for m, (kind, q) in enumerate(self.steps):
            kind.fetch(q, self.fetched.at[m])

    def spread(self, m):
        def act(kind, q, m):
            own, target = kind.own(q), kind.region(q, kind.me)
            local(own, own, self.fetched.at[m]).wait()
            for n, device in ((1, self.place.over_x), (2, self.place.over_y), (0, self.place.core)):
                self.push(m, n, target, device, own)
            if kind.stage is not None:
                self.home(kind, q, m).start()

        self.each(m, act)

    def forward(self, m):
        def act(kind, q, m):
            for p, device in enumerate((self.place.over_y, self.place.over_x)):
                owner = self.place.mine[1 + p]
                region, part = kind.region(q, owner), kind.part(q, owner, p)
                self.landed(m, 1 + p, region)
                self.push(m, 4 + 2 * p, part, device)
                self.push(m, 3 + 2 * p, region, self.place.core)

        self.each(m, act)

    def cross(self, m):
        def act(kind, q, m):
            for p in PAIR:
                self.landed(m, 4 + 2 * p, kind.part(q, self.place.mine[3], p))
            self.push(m, 7, kind.region(q, self.place.mine[3]), self.place.core)

        self.each(m, act)

    def complete(self, m):
        def act(kind, q, m):
            for n, owner in zip((0, 3, 5, 7), self.place.others):
                self.landed(m, n, kind.region(q, owner))
            if kind.stage is not None:
                self.home(kind, q, m).wait()

        self.each(m, act)

    def finish(self):
        for m in range(len(self.steps) - 2, len(self.steps)):
            for n in range(8):
                self.gone(m, n)


class Gradients:
    @staticmethod
    def scratch(rows, D, rounds):
        return Reducer.scratch((rows, CH)) + Reducer.scratch((HALF, D)) + [V((rounds, UNIT, D), bf16), DMA((2, 2, 2)), DMA((rounds,)), DMA(TWO_THREE)]

    def __init__(self, place, refs, outs, pieces, rounds, early=None):
        n = Reducer.COUNT
        self.place, self.pieces, self.rounds = place, pieces, rounds
        self.wide = Reducer(place, refs[:n])
        self.down = Reducer(place, refs[n : n + n])
        self.down_out, self.out_sem, self.local_sem, self.cross_sem = refs[n + n :]
        self.outs, self.early = outs, early
        self.before = 0 if early is None else 1

    def put_wide(self, p, value):
        b, rows = odd(p), value.shape[0] // 8
        value = value.astype(bf16)
        for s in range(8):
            for part in PAIR:
                self.wide.all[b, odd(s), s // 2, part] = value[rows * s : rows * (s + 1), CH * part : CH * (part + 1)]

    def put_down(self, i, q, value):
        value = value.astype(bf16)
        for n in PAIR:
            for core in PAIR:
                for part in PAIR:
                    row = LANES * n + UNIT * core + HALF * part
                    self.down.all[odd(q), core, 2 * odd(i) + n, part] = value[row : row + HALF]

    def flags(self, p):
        return odd(p), p < 2, p + 2 >= self.pieces

    def wide_send(self, p):
        self.wide.send(*self.flags(p))

    def wide1(self, p):
        self.wide.after_core(*self.flags(p))

    def wide2(self, p):
        self.wide.after_first(*self.flags(p))

    def wide3(self, p):
        self.wide.after_second(*self.flags(p))

    def wide_outs(self, b, i, outs):
        return [
            local(self.wide.out.at[b, part, :, block(n, LANES)], outs[part].at[:, at(s, LANES)], self.out_sem.at[b, part, n])
            for part in PAIR
            for n, s in enumerate(groups_of(i))
        ]

    def wide_gone(self, p):
        wait(*self.wide_outs(odd(p), 0, self.outs))

    def wide4(self, p):
        unless(p < 2)(lambda: self.wide_gone(p - 2))
        self.wide.after_copy(*self.flags(p))
        if self.before:
            when(p == 0)(lambda: start(*self.wide_outs(0, LAST_CHUNK, self.early)))
        when(p >= self.before)(lambda: start(*self.wide_outs(odd(p), p - self.before, self.outs)))

    def round_flags(self, q):
        return odd(q), q < 2, q + 2 >= self.rounds

    def down_send(self, q):
        self.down.send(*self.round_flags(q))

    def down1(self, q):
        self.down.after_core(*self.round_flags(q))

    def down2(self, q):
        self.down.after_first(*self.round_flags(q))

    def down3(self, q):
        self.down.after_second(*self.round_flags(q))

    def down_copies(self, q, j, outs, n):
        unit = 2 * j + self.place.c
        target = outs[2].at[block(unit % 5, UNIT), :]
        cross = remote(self.down_out.at[q], target, self.cross_sem.at[0, n], self.cross_sem.at[1, n], self.place.core)
        return unit // 5 == self.place.c, local(self.down_out.at[q], target, self.local_sem.at[q]), cross

    def down_start(self, q, j, outs, n):
        mine, here, cross = self.down_copies(q, j, outs, n)
        when(mine)(here.start)
        unless(mine)(cross.start)

    def down4(self, q):
        self.down.after_copy(*self.round_flags(q))
        for part in PAIR:
            self.down_out[q, block(part, HALF), :] = self.down.out[odd(q), part]
        j = q - self.before
        if self.before:
            when(q == 0)(lambda: self.down_start(q, LAST_ROUND, self.early, 2))
        when(j >= 0)(lambda: self.down_start(q, j, self.outs, j % 3))

    def squares(self):
        refs = (self.wide.squares, self.down.squares)
        return sum(ref[:, block(n, LANES)] for ref in refs for n in range(ref.shape[1] // LANES))

    def finish(self):
        for p in (self.pieces - 2, self.pieces - 1):
            self.wide_gone(p)
        for q in range(self.rounds):
            j, outs = q - self.before, self.outs
            n = j % 3
            if j < 0:
                j, outs, n = LAST_ROUND, self.early, 2
            mine, here, cross = self.down_copies(q, j, outs, n)
            when(mine)(here.wait)
            unless(mine)(cross.wait_send)
            theirs = (2 * j + 1 - self.place.c) // 5
            when(theirs == self.place.c)(cross.wait_recv)


def forward_kernel(h_hbm, wg_hbm, wu_hbm, wd_hbm, kept_hbm, out_hbm, a_hbm, aT_hbm, turned_hbm, down_hbm, next_wide_hbm, next_down_hbm,
                   a_ref, act_ref, wgu, wd, wide_stage, down_stage, gus, turn, hin, hout, aout, aTout, hsem, gsem, tsem, xsem, osem, dsem, *refs):
    T, D = a_ref.shape
    F = act_ref.shape[1]
    TILE = gus.shape[1]
    NC, NT, parts = F // CH, T // TILE, TILE // SUB
    place = Place()
    pair = (wg_hbm, wu_hbm)
    ones, downs, last_down = WideSteps(pair, 0, wgu, place.s), DownSteps(wd_hbm, 0, wd, place.s, 2), DownSteps(wd_hbm, 0, wd, place.s)
    gatherer = Gatherer(
        place,
        tuple((ones, i) for i in range(NC))
        + ((downs, 0), (downs, 2), (last_down, 4))
        + ((DownSteps(wd_hbm, 1, next_down_hbm, place.s, 2, down_stage), 0), (WideSteps(pair, 1, next_wide_hbm, place.s, 2, wide_stage), 0)),
        refs,
    )
    spread, forward, cross, complete = gatherer.spread, gatherer.forward, gatherer.cross, gatherer.complete

    def gather(plan):
        for name, m in re.findall("([sfxc])([0-9]+)", plan):
            {"s": spread, "f": forward, "x": cross, "c": complete}[name](int(m))

    def follow(plans, t, few=5):
        plans = plans.split("/")

        def one_of(first):
            for k, plan in enumerate(plans[first : first + few]):
                if plan:
                    branch(t == first + k)(lambda: gather(plan))

        for first in range(0, len(plans), few):
            branch(both(t >= first, t < first + few))(lambda: one_of(first))

    def load(t):
        rows = block(t, ROWS)
        return local(h_hbm.at[rows, :], a_ref.at[rows, :], hsem.at[t])

    def save(n):
        return local(gus.at[odd(n)], kept_hbm.at[n // NT, block(n % NT, TILE), :], gsem.at[odd(n)])

    def turned(t):
        return local(turn.at[odd(t)], turned_hbm.at[:, block(t, ROWS)], tsem.at[odd(t)])

    gatherer.fetch_all()
    loop(T // ROWS, lambda t: load(t).start())
    place.barrier(across=False)
    def norm(t):
        load(t).wait()
        rows = block(t, ROWS)
        a = normed(wide(a_ref[rows, :]))
        a_ref[rows, :] = a
        unless(t < 2)(lambda: turned(t - 2).wait())
        turn[odd(t)] = a.T
        turned(t).start()

    for k, plan in enumerate(NORM_PLAN.split("/")):
        gather(plan)
        loop(4 * k + 4, norm, 4 * k)

    def tile(n):
        i, t, b = n // NT, n % NT, odd(n)
        follow(TILE_PLAN, n)
        unless(n < 2)(lambda: save(n - 2).wait())

        def dots(k):
            gu = dot(a_ref[block(parts * t + k, SUB), :], wgu[i])
            gus[b, block(k, SUB), :] = gu
            return gu

        def elementwise(k, gu):
            gate, up = gu[:, :CH], gu[:, CH:]
            act = (gate * sigmoid(gate) * up).astype(bf16)
            for run, s in enumerate(groups_of(i)):
                act_ref[block(parts * t + k, SUB), at(s, LANES)] = act[:, LANES * run : LANES * (run + 1)]

        gu = dots(0)
        for k in range(parts):
            following = dots(k + 1) if k + 1 < parts else None
            elementwise(k, gu)
            gu = following
        save(n).start()

    loop(NC * NT, tile)
    gather(DOWN_PLAN.split("/")[0])
    down_out = local(wd, down_hbm, dsem)
    down_out.start()

    def inputs(t):
        return local(h_hbm.at[block(t, SUB), :], hin.at[odd(t)], xsem.at[odd(t)])

    def outputs(t):
        b, rows = odd(t), block(t, SUB)
        return local(hout.at[b], out_hbm.at[rows, :], osem.at[b, 0])

    def norms(t):
        b, rows = odd(t), block(t, SUB)
        return local(aout.at[b], a_hbm.at[rows, :], osem.at[b, 1]), local(aTout.at[b], aT_hbm.at[:, rows], osem.at[b, 2])

    count = T // SUB

    def norm_next(t):
        b = odd(t)
        a = normed(wide(hout[b]))
        aout[b] = a
        aTout[b] = a.T
        start(*norms(t))

    def down(t):
        branch(t > 0)(lambda: follow(DOWN_PLAN, t))
        b = odd(t)
        inputs(t).wait()
        when(t + 1 < count)(lambda: inputs(t + 1).start())
        unless(t < 2)(lambda: outputs(t - 2).wait())
        unless(t < 3)(lambda: wait(*norms(t - 3)))
        before = normed(wide(hout[1 - b]))
        aout[1 - b] = before
        aTout[1 - b] = before.T
        out = dot(act_ref[block(t, SUB), :], wd[...]).astype(bf16)
        hout[b] = (wide(hin[b]) + wide(out)).astype(bf16)
        outputs(t).start()
        unless(t < 1)(lambda: start(*norms(t - 1)))

    inputs(0).start()
    hout[1] = jnp.zeros_like(hout[1])
    loop(count, down)
    wait(*norms(count - 3))
    norm_next(count - 1)
    gather(END_PLAN)
    for n in (NC * NT - 2, NC * NT - 1):
        save(n).wait()
    for t in PAIR:
        turned(T // ROWS - 2 + t).wait()
        wait(outputs(count - 2 + t), *norms(count - 2 + t))
    down_out.wait()
    gatherer.finish()


def silu_back(dact, gate, up, act_ref, dgu_ref, rows):
    dact = wide(dact.astype(bf16))
    sg = sigmoid(gate)
    silu = gate * sg
    act_ref[rows, :] = (silu * up).astype(bf16)
    dgate = (dact * up * (sg + silu * (1.0 - sg))).astype(bf16)
    dup = (dact * silu).astype(bf16)
    dgu_ref[rows, block(0, CH)] = dgate
    dgu_ref[rows, block(1, CH)] = dup
    return dgate, dup


def middle_kernel(h_hbm, a_hbm, aT_hbm, dy_hbm, wg_hbm, wu_hbm, wd_hbm, wide_in, down_in, gg_hbm, gu_hbm, gd_hbm, dh_hbm, sq_hbm, wide_left, down_left, wide_hbm, down_hbm,
                  a_ref, aT_ref, dy_ref, da_ref, dgu_ref, act_ref, wgu, wd, sq, wide_stage, down_stage, hsem, asem, ysem, tsem, wsem, qsem, left_sem, *refs):
    T, D = a_ref.shape
    F = wg_hbm.shape[2]
    NC, NT = F // CH, T // TM
    n_blocks = T // ROWS

    def load(t):
        rows = block(t, ROWS)
        return local(h_hbm.at[rows, :], a_ref.at[rows, :], hsem.at[t])

    def states(t):
        rows = block(t, TM)
        return local(a_hbm.at[rows, :], a_ref.at[rows, :], asem.at[t]), local(dy_hbm.at[rows, :], dy_ref.at[rows, :], ysem.at[t])

    turned = local(aT_hbm, aT_ref, tsem)

    def weights(i):
        b = odd(i)
        return [local(wide_hbm.at[i], wgu.at[b], wsem.at[b, 2])] + rows_in(down_hbm, wd.at[b], wsem.at[b], i)

    start(*states(0))
    start(*weights(0))
    for t in range(1, NT):
        start(*states(t))
    turned.start()
    place = Place()
    gradients = Gradients(place, refs[Gatherer.COUNT :], (gg_hbm, gu_hbm, gd_hbm), NC - 1, NC // 2 - 1)
    wides = WideSteps((wg_hbm, wu_hbm), 1, wide_hbm, place.s, 2, wide_stage, 2)
    downs, last_down = (DownSteps(wd_hbm, 1, down_hbm, place.s, span, down_stage, 2) for span in (2, 1))
    gatherer = Gatherer(place, ((downs, 2), (wides, 2), (last_down, 4), (wides, 4), (wides, 6), (wides, 8)), refs[: Gatherer.COUNT])
    gatherer.fetch_all()
    place.barrier()
    gatherer.spread(0)

    def clear(t):
        da_ref[block(t, ROWS), :] = jnp.zeros((ROWS, D), f32)

    loop(n_blocks, clear)

    def gather_start():
        gatherer.forward(0)
        gatherer.spread(1)

    def gather_first(i):
        branch(i >= 1)(lambda: gatherer.cross(i))
        branch(i >= 1)(lambda: gatherer.spread(i + 1))

    def gather_last(i):
        branch(i == 0)(lambda: gatherer.cross(0))
        branch(i >= 1)(lambda: gatherer.forward(i + 1))
        branch(i >= 1)(lambda: gatherer.complete(i))

    def gather_between(i):
        branch(i == 0)(lambda: gatherer.complete(0))
        branch(i == 0)(lambda: gatherer.forward(1))

    def in_tiles(i):
        branch(i >= 1)(lambda: gradients.wide1(i - 1))
        branch(i >= 3)(lambda: gradients.wide4(i - 3))

    wide_over = local(gradients.wide.all.at[odd(NC - 1)], wide_left, left_sem.at[0])
    down_over = local(gradients.down.all.at[odd(NC // 2 - 1)], down_left, left_sem.at[1])

    def after_down(i):
        j = i // 2

        def odd_one():
            branch(i >= 3)(lambda: gradients.down4(j - 1))
            branch(i < NC - 1)(lambda: gradients.down_send(j))
            when(i == NC - 1)(down_over.start)

        branch(odd(i) == 1)(odd_one)
        branch(both(odd(i) == 0, i >= 2))(lambda: gradients.down2(j - 1))
        branch(i >= 2)(lambda: gradients.wide3(i - 2))

    def after_wide(i):
        j = i // 2
        branch(i < NC - 1)(lambda: gradients.wide_send(i))
        when(i == NC - 1)(wide_over.start)
        branch(i >= 1)(lambda: gradients.wide2(i - 1))
        branch(both(odd(i) == 1, i < NC - 1))(lambda: gradients.down1(j))
        branch(both(odd(i) == 0, i >= 2))(lambda: gradients.down3(j - 1))

    def chunk(i):
        b = odd(i)
        wait(*weights(i))

        def tile(t):
            when(i == 0)(lambda: wait(*states(t)))
            branch(t == 0)(lambda: gather_first(i))
            branch(both(t == 1, i == 0))(lambda: gather_start())
            branch(t == 2)(lambda: in_tiles(i))
            branch(t == 3)(lambda: gather_last(i))

            def dots(k):
                rows = block(2 * t + k, SUB)
                return dot(a_ref[rows, :], wgu[b]), dot_nt(dy_ref[rows, :], wd[b])

            def elementwise(k, gu, dact):
                return jnp.concatenate(silu_back(dact, gu[:, :CH], gu[:, CH:], act_ref, dgu_ref, block(2 * t + k, SUB)), 1)

            def back(k, dgu):
                da_ref[block(2 * t + k, SUB), :] += dot_nt(dgu, wgu[b])

            now = dots(0)
            following = dots(1)
            dgu = elementwise(0, *now)
            dgu_next = elementwise(1, *following)
            back(0, dgu)
            back(1, dgu_next)

        loop(NT, tile)
        gradients.put_down(i, i // 2, dot_tn(act_ref[...], dy_ref[...]))
        after_down(i)
        gather_between(i)
        when(i + 1 < NC)(lambda: start(*weights(i + 1)))
        when(i == 0)(turned.wait)
        gradients.put_wide(i, dot(aT_ref[...], dgu_ref[...]))
        after_wide(i)

    loop(NC, chunk)
    loop(n_blocks, lambda t: load(t).start())

    def store(t):
        rows = block(t, ROWS)
        return local(dy_ref.at[rows, :], dh_hbm.at[rows, :], hsem.at[t])

    def norm_back(t):
        rows = block(t, ROWS)
        load(t).wait()
        w = wide(a_ref[rows, :])
        da = wide(da_ref[rows, :].astype(bf16))
        scale = norm_scale(w)
        along = jnp.sum(da * w, -1, keepdims=True) * (scale * scale * scale) * (1.0 / D)
        by_h = (da * scale - w * along).astype(bf16)
        dy_ref[rows, :] = (wide(dy_ref[rows, :]) + wide(by_h)).astype(bf16)
        store(t).start()
        branch(t == n_blocks // 2)(lambda: gradients.wide3(NC - 2))

    gradients.wide4(NC - 3)
    loop(n_blocks, norm_back)
    gradients.wide4(NC - 2)
    sq[...] = gradients.squares()
    done = local(sq, sq_hbm, qsem)
    done.start()
    loop(n_blocks, lambda t: store(t).wait())
    gradients.finish()
    gatherer.finish()
    wait(wide_over, down_over)
    done.wait()


def last_kernel(aT_hbm, dy_hbm, kept_hbm, wd_hbm, sq_in, wide_left, down_left, eg_in, eu_in, ed_in, gg_hbm, gu_hbm, gd_hbm, sq_hbm, eg_hbm, eu_hbm, ed_hbm,
                aT_ref, dy_ref, even_dgu, even_act, odd_dgu, odd_act, by_gu, by_d, gus, wd, sq, parts, ysem, tsem, gsem, wsem, qsem, psem, left_sem, *refs):
    D, T = aT_ref.shape
    F = wd_hbm.shape[0]
    NC, NT = F // CH, T // TM
    depth = gus.shape[0]

    def states(t):
        rows = block(t, TM)
        return local(dy_hbm.at[rows, :], dy_ref.at[rows, :], ysem.at[t])

    def turned(t):
        rows = block(t, TM)
        return local(aT_hbm.at[:, rows], aT_ref.at[:, rows], tsem.at[t])

    def weights(i):
        b = odd(i)
        return rows_in(wd_hbm, wd.at[b], wsem.at[b], i)

    def kept(n):
        return local(kept_hbm.at[n // NT, block(n % NT, TM), :], gus.at[n % depth], gsem.at[n % depth])

    start(*weights(0))
    for t in range(NT):
        start(states(t), turned(t))
        if t < depth:
            kept(t).start()
    before = local(sq_in, sq, qsem)
    before.start()
    place = Place()
    gradients = Gradients(place, refs, (gg_hbm, gu_hbm, gd_hbm), NC + 1, NC // 2 + 1, (eg_hbm, eu_hbm, ed_hbm))
    left = [local(x, r.all.at[0], left_sem.at[n]) for n, (x, r) in enumerate(((wide_left, gradients.wide), (down_left, gradients.down)))]
    start(*left)
    place.barrier(all_peers=True)

    def add(ref, term, fresh):
        ref[...] = (ref[...] if fresh is None else jnp.where(fresh, 0.0, ref[...])) + term

    def terms_gu(t, dgu_ref, fresh=None):
        add(by_gu, dot(aT_ref[:, block(t, TM)], dgu_ref[...]), fresh)

    def terms_d(t, act_ref, fresh=None):
        add(by_d, dot_tn(act_ref[...], dy_ref[block(t, TM), :]), fresh)

    def ended(i):
        q = i // 2 + 1
        gradients.put_down(i, q, by_d[...])
        gradients.put_wide(i + 1, by_gu[...])
        gradients.wide_send(i + 1)
        branch(odd(i) == 1)(lambda: gradients.down_send(q))

    def step(n, now, before):
        some = before is not None
        i, t = n // NT, n % NT
        q = i // 2
        when(n < NT)(lambda: states(t).wait())
        if some:
            when(n <= NT)(lambda: turned(n - 1).wait())

        def next_weights():
            wait(*weights(i))
            when(i + 1 < NC)(lambda: start(*weights(i + 1)))

        when(t == 0)(next_weights)
        kept(n).wait()
        last = (t + NT - 1) % NT
        fresh = last == 0 if before is evens else None

        def dots(k):
            return dot_nt(dy_ref[block(2 * t + k, SUB), :], wd[odd(i)])

        def elementwise(k, dact):
            rows = block(k, SUB)
            silu_back(dact, gus[n % depth, rows, block(0, CH)], gus[n % depth, rows, block(1, CH)], now[1], now[0], rows)

        dact = dots(0)
        if some:
            terms_d(last, before[1], fresh)
        following = dots(1)
        elementwise(0, dact)
        if some:
            terms_gu(last, before[0], fresh)
        elementwise(1, following)
        when(n + depth < NC * NT)(lambda: kept(n + depth).start())

        def first_point():
            branch(both(odd(i) == 0, i >= 2))(lambda: gradients.down4(q - 1))
            branch(i >= 1)(lambda: ended(i - 1))
            branch(odd(i) == 1)(lambda: gradients.down2(q))

        def second_point():
            gradients.wide1(i)
            branch(i >= 1)(lambda: gradients.wide3(i - 1))

        def third_point():
            branch(odd(i) == 0)(lambda: gradients.down1(q))
            branch(odd(i) == 1)(lambda: gradients.down3(q))

        def fourth_point():
            gradients.wide2(i)
            branch(i >= 1)(lambda: gradients.wide4(i - 1))

        if some:
            for turn_at, act in enumerate((first_point, second_point, third_point, fourth_point)):
                branch(t == turn_at)(act)

    evens, odds = (even_dgu, even_act), (odd_dgu, odd_act)

    def two_steps(p):
        step(2 * p + 1, odds, evens)
        step(2 * p + 2, evens, odds)

    wait(*left)
    gradients.wide_send(0)
    gradients.down_send(0)
    step(0, evens, None)
    loop(NC * NT // 2 - 1, two_steps)
    step(NC * NT - 1 + place.s * 0, odds, evens)
    end, q = NC, NC // 2
    terms_d(NT - 1, odd_act)
    terms_gu(NT - 1, odd_dgu)
    gradients.down4(q - 1)
    ended(NC - 1)
    gradients.wide3(end - 1)
    before.wait()
    gradients.wide1(end)
    gradients.down1(q)
    gradients.wide4(end - 1)
    gradients.wide2(end)
    gradients.down2(q)
    gradients.wide3(end)
    gradients.down3(q)
    gradients.wide4(end)
    gradients.down4(q)
    sq[...] += gradients.squares()
    exchanges = [remote(sq, parts.at[n], psem.at[0, n], psem.at[1, n], {"s": s}) for n, s in enumerate(place.peers)]
    start(*exchanges)
    wait(*exchanges)
    sq[...] += sum(parts[n] for n in range(len(exchanges)))
    done = local(sq, sq_hbm, qsem)
    done.start()
    gradients.finish()
    done.wait()


def call(kernel, number, outs, scratch, inputs, aliases=None):
    return pl.pallas_call(
        kernel,
        out_shape=[jax.ShapeDtypeStruct(*o) for o in outs],
        in_specs=[ANY] * len(inputs),
        out_specs=[ANY] * len(outs),
        scratch_shapes=scratch,
        input_output_aliases=aliases or {},
        compiler_params=pltpu.CompilerParams(vmem_limit_bytes=VMEM_LIMIT, has_side_effects=True, collective_id=number),
    )(*inputs)


def forward(h, wg, wu, wd):
    (T, D), F = h.shape, wg.shape[2]
    chunks, down, states, turned = ((F // CH, D, BOTH), bf16), ((F, D), bf16), ((T, D), bf16), ((D, T), bf16)
    return call(
        forward_kernel,
        1,
        [((F // CH, T, BOTH), f32), states, states, turned, turned, down, chunks, down],
        [V(*states), V((T, F), bf16), V(*chunks), V(*down), V((2, D // 8, BOTH), bf16), V((2 * UNIT, D), bf16)]
        + [V((2, 2 * TM, BOTH), f32), V((2, D, ROWS), bf16), *[V(TWO + size, bf16) for size in [(SUB, D)] * 3 + [(D, SUB)]]]
        + [DMA((T // ROWS,)), DMA(TWO), DMA(TWO), DMA(TWO), DMA(TWO_THREE), DMA(())]
        + Gatherer.scratch(15),
        (h, wg, wu, wd),
    )


def middle(h, a, aT, dy, wg, wu, wd, chunks, down):
    (T, D), F = h.shape, wg.shape[2]
    mine, states = ((D // 8, F), bf16), ((T, D), bf16)
    return call(
        middle_kernel,
        2,
        [mine, mine, ((F // 8, D), bf16), states, (SMALL, f32)]
        + [((2, 4, 2) + size, bf16) for size in ((D // 8, CH), (HALF, D))]
        + [(chunks.shape, bf16), (down.shape, bf16)],
        [V(*states), V((D, T), bf16), V(*states), V((T, D), f32), V((T, BOTH), bf16), V((T, CH), bf16)]
        + [V((2, D, BOTH), bf16), V((2, CH, D), bf16), V(SMALL, f32), V((8, D // 8, BOTH), bf16), V((3 * UNIT, D), bf16)]
        + [DMA((T // ROWS,)), DMA((T // TM,)), DMA((T // TM,)), DMA(()), DMA(TWO_THREE), DMA(()), DMA(TWO)]
        + Gatherer.scratch(6)
        + Gradients.scratch(D // 8, D, F // CH // 2 - 1),
        (h, a, aT, dy, wg, wu, wd, chunks, down),
        {7: 7, 8: 8},
    )


def last(aT, dy, kept, wd, squares, wide_left, down_left, early):
    (D, T), F = aT.shape, wd.shape[0]
    mine = ((D // 8, F), bf16)
    return call(
        last_kernel,
        3,
        [mine, mine, ((F // 8, D), bf16), (SMALL, f32)] + [(g.shape, bf16) for g in early],
        [V((D, T), bf16), V((T, D), bf16), V((TM, BOTH), bf16), V((TM, CH), bf16), V((TM, BOTH), bf16), V((TM, CH), bf16), V((D, BOTH), f32), V((CH, D), f32)]
        + [V((3, TM, BOTH), f32), V((2, CH, D), bf16), V(SMALL, f32), V((7,) + SMALL, f32)]
        + [DMA((T // TM,)), DMA((T // TM,)), DMA((3,)), DMA((2, 2)), DMA(()), DMA((2, 7)), DMA(TWO)]
        + Gradients.scratch(D // 8, D, F // CH // 2 + 1),
        (aT, dy, kept, wd, squares, wide_left, down_left, *early),
        dict(zip(range(7, 10), range(4, 7))),
    )


def adamw(w, m, v, g):
    m = 0.9 * m + 0.1 * g
    v = 0.95 * v + 0.05 * g * g
    step = m * lax.rsqrt(v + 1e-8) + 0.1 * w
    return (w - 0.02 * step).astype(bf16), m, v


def update_kernel(count, sq_hbm, *refs):
    sources, targets, buffers, (sq, in_sem, out_sem, sq_sem) = refs[:15], refs[15:24], refs[24:36], refs[36:]
    units = [(layer, k) for layer in PAIR for k in range(3)]

    def buffer(which, layer, k):
        return buffers[3 * which + k].at[layer]

    def loads(layer, k):
        hbm = [sources[6 + 3 * which + k].at[layer] for which in range(3)] + [sources[3 * layer + k]]
        return [local(source, buffer(which, layer, k), in_sem.at[which, layer, k]) for which, source in enumerate(hbm)]

    def stores(layer, k):
        return [local(buffer(which, layer, k), targets[3 * which + k].at[layer], out_sem.at[which, layer, k]) for which in range(3)]

    size = local(sq_hbm, sq, sq_sem)
    size.start()
    for unit in units:
        start(*loads(*unit))
    size.wait()
    factor = jnp.minimum(1.0, 0.5 * lax.rsqrt(jnp.full((1, 1), jnp.sum(sq[...]) / count + 1e-30, f32)))
    for unit in units:
        wait(*loads(*unit))
        w, m, v, g = (buffer(which, *unit) for which in range(4))

        def take_step(t):
            rows = block(t, 16)
            w[rows, :], m[rows, :], v[rows, :] = adamw(wide(w[rows, :]), m[rows, :], v[rows, :], wide(g[rows, :]) * factor)

        loop(w.shape[0] // 16, take_step)
        start(*stores(*unit))
    for unit in units:
        wait(*stores(*unit))


def update(squares, count, firsts, seconds, weights, m, v):
    shapes = [jax.ShapeDtypeStruct(w.shape, kind) for kind in (bf16, f32, f32) for w in weights]
    return pl.pallas_call(
        functools.partial(update_kernel, count),
        out_shape=shapes,
        in_specs=[ANY] * 16,
        out_specs=[ANY] * len(shapes),
        scratch_shapes=[V(x.shape, x.dtype) for x in shapes + shapes[:3]] + [V(SMALL, f32), DMA((4, 2, 3)), DMA((3, 2, 3)), DMA(())],
        compiler_params=pltpu.CompilerParams(vmem_limit_bytes=VMEM_LIMIT),
    )(squares, *firsts, *seconds, *weights, *m, *v)


def solution(mesh):
    def step(x, dy, *arrays):
        weights, m, v = (arrays[i : i + 3] for i in (0, 3, 6))
        kept, h, a1, a1T, a0T, down0, chunks1, down1 = forward(x[0], *weights)
        *early, by_h, squares, wide_left, down_left, _, _ = middle(h, a1, a1T, dy[0], *weights, chunks1, down1)
        *first_sums, squares, gate1, up1, down_1 = last(a0T, by_h, kept, down0, squares, wide_left, down_left, early)
        count = lax.psum(1, "s") * sum(w.size for w in weights)
        return tuple(update(squares, count, first_sums, (gate1, up1, down_1), weights, m, v))

    states, cut = P(("rep", "r", "s"), None, None), P(None, "s", None)
    return jax.shard_map(
        step,
        mesh=mesh,
        in_specs=(states, states) + (cut,) * 9,
        out_specs=(P("rep", "s", None),) * 9,
        check_vma=False,
    )
```

```python
import functools
import re

import jax
import jax.numpy as jnp
from jax import lax
from jax.experimental import pallas as pl
from jax.experimental.pallas import tpu as pltpu
from jax.sharding import PartitionSpec as P

bf16, f32 = jnp.bfloat16, jnp.float32
CH, SUB, TM, LANES, ROWS, UNIT = 256, 512, 1024, 128, 256, 64
HALF, BOTH = UNIT // 2, 2 * CH
SMALL, TWO, TWO_THREE = (8, LANES), (2,), (2, 3)
PAIR = range(2)
NT_DIMS = (((1,), (1,)), ((), ()))
TN_DIMS = (((0,), (0,)), ((), ()))
VMEM_LIMIT = 67043328
MESH = pl.DeviceIdType.MESH
EPS = 1e-6
LAST_CHUNK, LAST_ROUND = 9, 4
ANY = pl.BlockSpec(memory_space=pl.ANY)
V, DMA, REGULAR = pltpu.VMEM, pltpu.SemaphoreType.DMA, pltpu.SemaphoreType.REGULAR
local = pltpu.make_async_copy


NORM_PLAN = "s0s1//s2/"
TILE_PLAN = "".join((
    "f0x0c0f1f2s3/s4/x1c1x2s5/c2f3s6/f4/",
    "x3f5s7/c3f6x4s8/c4x5s9/c5x6f7/c6f8s10/",
    "f9/x7x8/c7c8s11/x9f10/c9s12/",
    "f11/x10s13/c10f12/x11/c11s14/",
))
DOWN_PLAN = "x12c12f13//f14/x13/c13x14/c14//"
END_PLAN = ""


def odd(i):
    return i % 2


def groups_of(i):
    first = i // 2 + 10 * odd(i)
    return first * LANES, (first + 5) * LANES


def dot(a, b):
    return jnp.dot(a, b, preferred_element_type=f32)


def dot_nt(a, b):
    return lax.dot_general(a, b, NT_DIMS, preferred_element_type=f32)


def dot_tn(a, b):
    return lax.dot_general(a, b, TN_DIMS, preferred_element_type=f32)


def at(start, size, multiple=None):
    return pl.ds(pl.multiple_of(start, multiple or size), size)


def block(t, size):
    return at(t * size, size)


def wide(x):
    return x.astype(f32)


def sigmoid(x):
    return 1.0 / (1.0 + jnp.exp(-x))


def start(*copies):
    for c in copies:
        c.start()


def wait(*copies):
    for c in copies:
        c.wait()


def loop(count, body, first=0):
    def turn(t, carry):
        body(t)
        return carry

    lax.fori_loop(first, count, turn, 0)


def when(condition):
    if isinstance(condition, bool):
        return (lambda f: f()) if condition else (lambda f: None)
    return pl.when(condition)


def unless(condition):
    return when(not condition if isinstance(condition, bool) else jnp.logical_not(condition))


def branch(condition):
    if isinstance(condition, bool):
        return when(condition)
    return lambda f: loop(condition.astype(jnp.int32), lambda _: f())


def both(a, b):
    return a and b if isinstance(a, bool) and isinstance(b, bool) else jnp.logical_and(a, b)


def rows_in(w_hbm, buf, sem, i):
    return [local(w_hbm.at[at(s, LANES), :], buf.at[block(n, LANES), :], sem.at[n]) for n, s in enumerate(groups_of(i))]


def norm_scale(w):
    return lax.rsqrt(jnp.mean(w * w, -1, keepdims=True) + EPS)


def normed(w):
    return (w * norm_scale(w)).astype(bf16)


class Place:
    def __init__(self):
        self.s = s = lax.axis_index("s")
        self.c, self.y, self.x = odd(s), odd(s // 2), s // 4
        other, across_x, across_y = 1 - 2 * self.c, 4 - 8 * self.x, 2 - 4 * self.y
        self.core, self.over_x, self.over_y = {"s": s + other}, {"s": s + across_x}, {"s": s + across_y}
        self.over_z = {"r": 1 - lax.axis_index("r")}
        self.mine = (s, s + across_x, s + across_y, s + across_x + across_y)
        self.others = tuple(o + other for o in self.mine)
        self.peers = self.mine[1:] + self.others

    def barrier(self, across=True, all_peers=False):
        barrier = pltpu.get_barrier_semaphore()
        neighbours = [{"s": s} for s in self.peers] if all_peers else [self.core, self.over_y, self.over_x]
        if across:
            neighbours.append(self.over_z)
        for device in neighbours:
            give(barrier, device)
        pl.semaphore_wait(barrier, len(neighbours))


def remote(source, target, send, receive, device):
    return pltpu.make_async_remote_copy(source, target, send, receive, device_id=device, device_id_type=MESH)


def give(semaphore, device):
    pl.semaphore_signal(semaphore, inc=1, device_id=device, device_id_type=MESH)


def take(semaphore):
    pl.semaphore_wait(semaphore, 1)


class Reducer:
    SHAPES = ("ocp", "cp", "pp", "pp", "p", "p", "p", "p", "p")

    @classmethod
    def scratch(cls, shape):
        sizes = {"o": (2, 4), "c": (4,), "p": (2,)}
        buffers = [V((2,) + sum((sizes[c] for c in lead if c != "c" or "o" not in lead), ()) + shape, bf16) for lead in cls.SHAPES]
        one, two = (2,), (2, 2)
        return buffers + [DMA((2,) + n) for n in (one, two, two, one)] + [REGULAR(n) for n in (one, two, two, one)] + [V((8, shape[1]), f32)]

    COUNT = 18

    def __init__(self, place, refs):
        self.place = place
        self.all, self.got0, self.out1, self.got1, self.out2, self.got2, self.out3, self.got3, self.out = refs[:9]
        self.sem0, self.sem1, self.sem2, self.sem3, self.free0, self.free1, self.free2, self.free3, self.squares = refs[9:]
        self.squares[...] = jnp.zeros_like(self.squares)
        self.first_way, self.second_way = (place.over_x, place.over_y), (place.over_y, place.over_x)

    def copy0(self, b):
        return remote(self.all.at[b, 1 - self.place.c], self.got0.at[b], self.sem0.at[0, b], self.sem0.at[1, b], self.place.core)

    def copy1(self, b, p):
        return remote(self.out1.at[b, p], self.got1.at[b, p], self.sem1.at[0, b, p], self.sem1.at[1, b, p], self.first_way[p])

    def copy2(self, b, p):
        return remote(self.out2.at[b, p], self.got2.at[b, p], self.sem2.at[0, b, p], self.sem2.at[1, b, p], self.second_way[p])

    def copy3(self, b):
        return remote(self.out3.at[b], self.got3.at[b], self.sem3.at[0, b], self.sem3.at[1, b], self.place.over_z)

    def chip_sum(self, b, p, x, y):
        k = 2 * x + y
        return wide(self.all[b, self.place.c, k, p]) + wide(self.got0[b, k, p])

    def send(self, b, first, final):
        unless(first)(lambda: take(self.free0.at[b]))
        self.copy0(b).start()

    def after_core(self, b, first, final):
        place = self.place
        self.copy0(b).wait()
        for p in PAIR:
            unless(first)(lambda: take(self.free1.at[b, p]))
            for n in PAIR:
                self.out1[b, p, n] = self.chip_sum(b, p, *((n, 1 - place.y) if p else (1 - place.x, n))).astype(bf16)
            self.copy1(b, p).start()

    def after_first(self, b, first, final):
        place = self.place
        for p in PAIR:
            self.copy1(b, p).wait()
            unless(first)(lambda: take(self.free2.at[b, p]))
            away = (1 - place.x, place.y) if p else (place.x, 1 - place.y)
            self.out2[b, p] = (self.chip_sum(b, p, *away) + wide(self.got1[b, p, away[1 - p]])).astype(bf16)
            self.copy2(b, p).start()

    def after_second(self, b, first, final):
        place = self.place
        for p in PAIR:
            self.copy2(b, p).wait()
            near = place.x if p else place.y
            self.out3[b, p] = (self.chip_sum(b, p, place.x, place.y) + wide(self.got1[b, p, near]) + wide(self.got2[b, p])).astype(bf16)
        unless(first)(lambda: take(self.free3.at[b]))
        self.copy3(b).start()

        def release():
            give(self.free0.at[b], place.core)
            for p in PAIR:
                give(self.free1.at[b, p], self.first_way[p])
                give(self.free2.at[b, p], self.second_way[p])

        unless(final)(release)

    def after_copy(self, b, first, final):
        self.copy3(b).wait()
        for p in PAIR:
            g = (wide(self.out3[b, p]) + wide(self.got3[b, p])).astype(bf16)
            self.out[b, p] = g
            g = wide(g)
            self.squares[...] += jnp.sum((g * g).reshape(-1, 8, g.shape[1]), 0)
        unless(final)(lambda: give(self.free3.at[b], self.place.over_z))


class Steps:
    def __init__(self, weights, layer, land, me, span=1, stage=None, first=0):
        self.weights, self.layer, self.land, self.me, self.span, self.stage, self.first = weights, layer, land, me, span, stage, first

    def own(self, q):
        return self.region(q, self.me) if self.stage is None else self.staged(q)


class WideSteps(Steps):
    @property
    def rows(self):
        return self.weights[0].shape[1]

    def region(self, q, owner):
        return self.land.at[pl.ds(q, self.span), at(self.rows * owner, self.rows, 16), :]

    def part(self, q, owner, p):
        return self.land.at[pl.ds(q, self.span), at(self.rows * owner, self.rows, 16), block(p, CH)]

    def staged(self, q):
        return self.stage.at[pl.ds(q - self.first, self.span)]

    def fetch(self, q, sem):
        for k in range(self.span):
            for p in PAIR:
                for n, s in enumerate(groups_of(q + k)):
                    lanes = at(CH * p + LANES * n, LANES)
                    if self.stage is None:
                        target = self.land.at[q + k, at(self.rows * self.me, self.rows, 16), lanes]
                    else:
                        target = self.stage.at[q + k - self.first, :, lanes]
                    local(self.weights[p].at[self.layer, :, at(s, LANES)], target, sem).start()


class DownSteps(Steps):
    @property
    def rows(self):
        return self.weights.shape[1]

    def region(self, q, owner):
        return self.land.at[at(self.rows * owner + UNIT * q, UNIT * self.span, UNIT), :]

    def part(self, q, owner, p):
        return self.land.at[at(self.rows * owner + UNIT * q + HALF * self.span * p, HALF * self.span, HALF), :]

    def staged(self, q):
        return self.stage.at[at(UNIT * (q - self.first), UNIT * self.span, UNIT), :]

    def fetch(self, q, sem):
        local(self.weights.at[self.layer, at(UNIT * q, UNIT * self.span, UNIT), :], self.own(q), sem).start()


class Gatherer:
    @staticmethod
    def scratch(steps):
        return [DMA((steps, 8)), DMA((2, 8)), DMA((steps,)), DMA((steps,))]

    COUNT = 4

    def __init__(self, place, steps, refs):
        self.place, self.steps = place, steps
        self.received, self.sent, self.fetched, self.homed = refs

    def each(self, m, f):
        for k, (kind, q) in enumerate(self.steps):
            branch(m == k)(functools.partial(f, kind, q, k))

    def copy(self, m, n, source, target, device):
        return remote(source, target, self.sent.at[odd(m), n], self.received.at[m, n], device)

    def push(self, m, n, region, device, source=None):
        copy = self.copy(m, n, region if source is None else source, region, device)
        if m >= 2:
            self.gone(m - 2, n)
        copy.start()

    def gone(self, m, n):
        kind, q = self.steps[m]
        region = kind.part(q, self.place.s, 0) if n in (4, 6) else kind.region(q, self.place.s)
        self.copy(m, n, region, region, self.place.core).wait_send()

    def landed(self, m, n, target):
        self.copy(m, n, target, target, self.place.core).wait_recv()

    def home(self, kind, q, m):
        return local(kind.own(q), kind.region(q, kind.me), self.homed.at[m])

    def fetch_all(self):
        for m, (kind, q) in enumerate(self.steps):
            kind.fetch(q, self.fetched.at[m])

    def spread(self, m):
        def act(kind, q, m):
            own, target = kind.own(q), kind.region(q, kind.me)
            local(own, own, self.fetched.at[m]).wait()
            for n, device in ((1, self.place.over_x), (2, self.place.over_y), (0, self.place.core)):
                self.push(m, n, target, device, own)
            if kind.stage is not None:
                self.home(kind, q, m).start()

        self.each(m, act)

    def forward(self, m):
        def act(kind, q, m):
            for p, device in enumerate((self.place.over_y, self.place.over_x)):
                owner = self.place.mine[1 + p]
                region, part = kind.region(q, owner), kind.part(q, owner, p)
                self.landed(m, 1 + p, region)
                self.push(m, 4 + 2 * p, part, device)
                self.push(m, 3 + 2 * p, region, self.place.core)

        self.each(m, act)

    def cross(self, m):
        def act(kind, q, m):
            for p in PAIR:
                self.landed(m, 4 + 2 * p, kind.part(q, self.place.mine[3], p))
            self.push(m, 7, kind.region(q, self.place.mine[3]), self.place.core)

        self.each(m, act)

    def complete(self, m):
        def act(kind, q, m):
            for n, owner in zip((0, 3, 5, 7), self.place.others):
                self.landed(m, n, kind.region(q, owner))
            if kind.stage is not None:
                self.home(kind, q, m).wait()

        self.each(m, act)

    def run(self, plan):
        for name, m in re.findall("([sfxc])([0-9]+)", plan):
            {"s": self.spread, "f": self.forward, "x": self.cross, "c": self.complete}[name](int(m))

    def follow(self, plans, t, few=5):
        plans = plans.split("/")

        def one_of(first):
            for k, plan in enumerate(plans[first : first + few]):
                if plan:
                    branch(t == first + k)(lambda: self.run(plan))

        for first in range(0, len(plans), few):
            branch(both(t >= first, t < first + few))(lambda: one_of(first))

    def finish(self):
        for m in range(len(self.steps) - 2, len(self.steps)):
            for n in range(8):
                self.gone(m, n)


class Gradients:
    @staticmethod
    def scratch(rows, D, rounds):
        return Reducer.scratch((rows, CH)) + Reducer.scratch((HALF, D)) + [V((rounds, UNIT, D), bf16), DMA((2, 2, 2)), DMA((rounds,)), DMA(TWO_THREE)]

    def __init__(self, place, refs, outs, pieces, rounds, early=None):
        n = Reducer.COUNT
        self.place, self.pieces, self.rounds = place, pieces, rounds
        self.wide = Reducer(place, refs[:n])
        self.down = Reducer(place, refs[n : n + n])
        self.down_out, self.out_sem, self.local_sem, self.cross_sem = refs[n + n :]
        self.outs, self.early = outs, early
        self.before = 0 if early is None else 1

    def put_wide(self, p, value):
        b, rows = odd(p), value.shape[0] // 8
        value = value.astype(bf16)
        for s in range(8):
            for part in PAIR:
                self.wide.all[b, odd(s), s // 2, part] = value[rows * s : rows * (s + 1), CH * part : CH * (part + 1)]

    def put_down(self, i, q, value):
        value = value.astype(bf16)
        for n in PAIR:
            for core in PAIR:
                for part in PAIR:
                    row = LANES * n + UNIT * core + HALF * part
                    self.down.all[odd(q), core, 2 * odd(i) + n, part] = value[row : row + HALF]

    def flags(self, p):
        return odd(p), p < 2, p + 2 >= self.pieces

    def wide_send(self, p):
        self.wide.send(*self.flags(p))

    def wide1(self, p):
        self.wide.after_core(*self.flags(p))

    def wide2(self, p):
        self.wide.after_first(*self.flags(p))

    def wide3(self, p):
        self.wide.after_second(*self.flags(p))

    def wide_outs(self, b, i, outs):
        return [
            local(self.wide.out.at[b, part, :, block(n, LANES)], outs[part].at[:, at(s, LANES)], self.out_sem.at[b, part, n])
            for part in PAIR
            for n, s in enumerate(groups_of(i))
        ]

    def wide_gone(self, p):
        wait(*self.wide_outs(odd(p), 0, self.outs))

    def wide4(self, p):
        unless(p < 2)(lambda: self.wide_gone(p - 2))
        self.wide.after_copy(*self.flags(p))
        if self.before:
            when(p == 0)(lambda: start(*self.wide_outs(0, LAST_CHUNK, self.early)))
        when(p >= self.before)(lambda: start(*self.wide_outs(odd(p), p - self.before, self.outs)))

    def round_flags(self, q):
        return odd(q), q < 2, q + 2 >= self.rounds

    def down_send(self, q):
        self.down.send(*self.round_flags(q))

    def down1(self, q):
        self.down.after_core(*self.round_flags(q))

    def down2(self, q):
        self.down.after_first(*self.round_flags(q))

    def down3(self, q):
        self.down.after_second(*self.round_flags(q))

    def down_copies(self, q, j, outs, n):
        unit = 2 * j + self.place.c
        target = outs[2].at[block(unit % 5, UNIT), :]
        cross = remote(self.down_out.at[q], target, self.cross_sem.at[0, n], self.cross_sem.at[1, n], self.place.core)
        return unit // 5 == self.place.c, local(self.down_out.at[q], target, self.local_sem.at[q]), cross

    def down_start(self, q, j, outs, n):
        mine, here, cross = self.down_copies(q, j, outs, n)
        when(mine)(here.start)
        unless(mine)(cross.start)

    def down4(self, q):
        self.down.after_copy(*self.round_flags(q))
        for part in PAIR:
            self.down_out[q, block(part, HALF), :] = self.down.out[odd(q), part]
        j = q - self.before
        if self.before:
            when(q == 0)(lambda: self.down_start(q, LAST_ROUND, self.early, 2))
        when(j >= 0)(lambda: self.down_start(q, j, self.outs, j % 3))

    def squares(self):
        refs = (self.wide.squares, self.down.squares)
        return sum(ref[:, block(n, LANES)] for ref in refs for n in range(ref.shape[1] // LANES))

    def finish(self):
        for p in (self.pieces - 2, self.pieces - 1):
            self.wide_gone(p)
        for q in range(self.rounds):
            j, outs = q - self.before, self.outs
            n = j % 3
            if j < 0:
                j, outs, n = LAST_ROUND, self.early, 2
            mine, here, cross = self.down_copies(q, j, outs, n)
            when(mine)(here.wait)
            unless(mine)(cross.wait_send)
            theirs = (2 * j + 1 - self.place.c) // 5
            when(theirs == self.place.c)(cross.wait_recv)


def forward_kernel(h_hbm, wg_hbm, wu_hbm, wd_hbm, kept_hbm, out_hbm, a_hbm, aT_hbm, turned_hbm, down_hbm, next_wide_hbm, next_down_hbm,
                   a_ref, act_ref, wgu, wd, wide_stage, down_stage, gus, turn, hin, hout, aout, aTout, hsem, gsem, tsem, xsem, osem, dsem, *refs):
    T, D = a_ref.shape
    F = act_ref.shape[1]
    TILE = gus.shape[1]
    NC, NT, parts = F // CH, T // TILE, TILE // SUB
    place = Place()
    pair = (wg_hbm, wu_hbm)
    ones, downs, last_down = WideSteps(pair, 0, wgu, place.s), DownSteps(wd_hbm, 0, wd, place.s, 2), DownSteps(wd_hbm, 0, wd, place.s)
    gatherer = Gatherer(
        place,
        tuple((ones, i) for i in range(NC))
        + ((downs, 0), (downs, 2), (last_down, 4))
        + ((DownSteps(wd_hbm, 1, next_down_hbm, place.s, 2, down_stage), 0), (WideSteps(pair, 1, next_wide_hbm, place.s, 2, wide_stage), 0)),
        refs,
    )
    gather, follow = gatherer.run, gatherer.follow

    def load(t):
        rows = block(t, ROWS)
        return local(h_hbm.at[rows, :], a_ref.at[rows, :], hsem.at[t])

    def save(n):
        return local(gus.at[odd(n)], kept_hbm.at[n // NT, block(n % NT, TILE), :], gsem.at[odd(n)])

    def turned(t):
        return local(turn.at[odd(t)], turned_hbm.at[:, block(t, ROWS)], tsem.at[odd(t)])

    gatherer.fetch_all()
    loop(T // ROWS, lambda t: load(t).start())
    place.barrier(across=False)
    def norm(t):
        load(t).wait()
        rows = block(t, ROWS)
        a = normed(wide(a_ref[rows, :]))
        a_ref[rows, :] = a
        unless(t < 2)(lambda: turned(t - 2).wait())
        turn[odd(t)] = a.T
        turned(t).start()

    for k, plan in enumerate(NORM_PLAN.split("/")):
        gather(plan)
        loop(4 * k + 4, norm, 4 * k)

    def tile(n):
        i, t, b = n // NT, n % NT, odd(n)
        follow(TILE_PLAN, n)
        unless(n < 2)(lambda: save(n - 2).wait())

        def dots(k):
            gu = dot(a_ref[block(parts * t + k, SUB), :], wgu[i])
            gus[b, block(k, SUB), :] = gu
            return gu

        def elementwise(k, gu):
            gate, up = gu[:, :CH], gu[:, CH:]
            act = (gate * sigmoid(gate) * up).astype(bf16)
            for run, s in enumerate(groups_of(i)):
                act_ref[block(parts * t + k, SUB), at(s, LANES)] = act[:, LANES * run : LANES * (run + 1)]

        gu = dots(0)
        for k in range(parts):
            following = dots(k + 1) if k + 1 < parts else None
            elementwise(k, gu)
            gu = following
        save(n).start()

    loop(NC * NT, tile)
    gather(DOWN_PLAN.split("/")[0])
    down_out = local(wd, down_hbm, dsem)
    down_out.start()

    def inputs(t):
        return local(h_hbm.at[block(t, SUB), :], hin.at[odd(t)], xsem.at[odd(t)])

    def outputs(t):
        b, rows = odd(t), block(t, SUB)
        return local(hout.at[b], out_hbm.at[rows, :], osem.at[b, 0])

    def norms(t):
        b, rows = odd(t), block(t, SUB)
        return local(aout.at[b], a_hbm.at[rows, :], osem.at[b, 1]), local(aTout.at[b], aT_hbm.at[:, rows], osem.at[b, 2])

    count = T // SUB

    def norm_next(t):
        b = odd(t)
        a = normed(wide(hout[b]))
        aout[b] = a
        aTout[b] = a.T
        start(*norms(t))

    def down(t):
        branch(t > 0)(lambda: follow(DOWN_PLAN, t))
        b = odd(t)
        inputs(t).wait()
        when(t + 1 < count)(lambda: inputs(t + 1).start())
        unless(t < 2)(lambda: outputs(t - 2).wait())
        unless(t < 3)(lambda: wait(*norms(t - 3)))
        before = normed(wide(hout[1 - b]))
        aout[1 - b] = before
        aTout[1 - b] = before.T
        out = dot(act_ref[block(t, SUB), :], wd[...]).astype(bf16)
        hout[b] = (wide(hin[b]) + wide(out)).astype(bf16)
        outputs(t).start()
        unless(t < 1)(lambda: start(*norms(t - 1)))

    inputs(0).start()
    hout[1] = jnp.zeros_like(hout[1])
    loop(count, down)
    wait(*norms(count - 3))
    norm_next(count - 1)
    gather(END_PLAN)
    for n in (NC * NT - 2, NC * NT - 1):
        save(n).wait()
    for t in PAIR:
        turned(T // ROWS - 2 + t).wait()
        wait(outputs(count - 2 + t), *norms(count - 2 + t))
    down_out.wait()
    gatherer.finish()


def silu_back(dact, gate, up, act_ref, dgu_ref, rows):
    dact = wide(dact.astype(bf16))
    sg = sigmoid(gate)
    silu = gate * sg
    act_ref[rows, :] = (silu * up).astype(bf16)
    dgate = (dact * up * (sg + silu * (1.0 - sg))).astype(bf16)
    dup = (dact * silu).astype(bf16)
    dgu_ref[rows, block(0, CH)] = dgate
    dgu_ref[rows, block(1, CH)] = dup
    return dgate, dup


def middle_kernel(h_hbm, a_hbm, aT_hbm, dy_hbm, wg_hbm, wu_hbm, wd_hbm, wide_in, down_in, gg_hbm, gu_hbm, gd_hbm, dh_hbm, sq_hbm, wide_left, down_left, wide_hbm, down_hbm,
                  a_ref, aT_ref, dy_ref, da_ref, dgu_ref, act_ref, wgu, wd, sq, wide_stage, down_stage, hsem, asem, ysem, tsem, wsem, qsem, left_sem, *refs):
    T, D = a_ref.shape
    F = wg_hbm.shape[2]
    NC, NT = F // CH, T // TM
    n_blocks = T // ROWS

    def load(t):
        rows = block(t, ROWS)
        return local(h_hbm.at[rows, :], a_ref.at[rows, :], hsem.at[t])

    def states(t):
        rows = block(t, TM)
        return local(a_hbm.at[rows, :], a_ref.at[rows, :], asem.at[t]), local(dy_hbm.at[rows, :], dy_ref.at[rows, :], ysem.at[t])

    turned = local(aT_hbm, aT_ref, tsem)

    def weights(i):
        b = odd(i)
        return [local(wide_hbm.at[i], wgu.at[b], wsem.at[b, 2])] + rows_in(down_hbm, wd.at[b], wsem.at[b], i)

    start(*states(0), *weights(0))
    place = Place()
    gradients = Gradients(place, refs[Gatherer.COUNT :], (gg_hbm, gu_hbm, gd_hbm), NC - 1, NC // 2 - 1)
    wides = WideSteps((wg_hbm, wu_hbm), 1, wide_hbm, place.s, 2, wide_stage, 2)
    downs, last_down = (DownSteps(wd_hbm, 1, down_hbm, place.s, span, down_stage, 2) for span in (2, 1))
    gatherer = Gatherer(place, ((downs, 2), (wides, 2), (last_down, 4), (wides, 4), (wides, 6), (wides, 8)), refs[: Gatherer.COUNT])
    gatherer.fetch_all()
    place.barrier()
    gatherer.spread(0)

    def clear(t):
        da_ref[block(t, ROWS), :] = jnp.zeros((ROWS, D), f32)

    loop(n_blocks, clear)

    def in_tiles(i):
        gatherer.follow("f0s1/x1s2", i)
        branch(i >= 1)(lambda: gradients.wide1(i - 1))
        branch(i >= 3)(lambda: gradients.wide4(i - 3))

    wide_over = local(gradients.wide.all.at[odd(NC - 1)], wide_left, left_sem.at[0])
    down_over = local(gradients.down.all.at[odd(NC // 2 - 1)], down_left, left_sem.at[1])

    def after_down(i):
        j = i // 2

        def odd_one():
            branch(i >= 3)(lambda: gradients.down4(j - 1))
            branch(i < NC - 1)(lambda: gradients.down_send(j))
            when(i == NC - 1)(down_over.start)

        branch(odd(i) == 1)(odd_one)
        branch(i == NC - 1)(lambda: gradients.wide2(i - 1))
        branch(both(odd(i) == 0, i >= 2))(lambda: gradients.down2(j - 1))
        branch(i >= 2)(lambda: gradients.wide3(i - 2))

    def after_wide(i):
        j = i // 2
        branch(i < NC - 1)(lambda: gradients.wide_send(i))
        branch(i == 0)(lambda: gatherer.run("c0f1"))
        when(i == NC - 1)(wide_over.start)
        branch(both(i >= 1, i < NC - 1))(lambda: gradients.wide2(i - 1))
        branch(i == NC - 1)(lambda: gradients.wide3(i - 1))
        branch(both(odd(i) == 1, i < NC - 1))(lambda: gradients.down1(j))
        branch(both(odd(i) == 0, i >= 2))(lambda: gradients.down3(j - 1))

    def chunk(i):
        b = odd(i)
        wait(*weights(i))

        def tile(t):
            def load_states():
                wait(*states(t))
                when(t + 1 < NT)(lambda: start(*states(t + 1)))
                when(t + 1 == NT)(turned.start)

            branch(i == 0)(load_states)
            branch(t == 0)(lambda: gatherer.follow("//x2s3/x3s4/x4s5/x5", i))
            branch(t == 2)(lambda: in_tiles(i))
            branch(t == 3)(lambda: gatherer.follow("/c1/f3c2/f4c3/f5c4/c5", i))

            def dots(k):
                rows = block(2 * t + k, SUB)
                return dot(a_ref[rows, :], wgu[b]), dot_nt(dy_ref[rows, :], wd[b])

            def elementwise(k, gu, dact):
                return jnp.concatenate(silu_back(dact, gu[:, :CH], gu[:, CH:], act_ref, dgu_ref, block(2 * t + k, SUB)), 1)

            def back(k, dgu):
                da_ref[block(2 * t + k, SUB), :] += dot_nt(dgu, wgu[b])

            now = dots(0)
            following = dots(1)
            dgu = elementwise(0, *now)
            dgu_next = elementwise(1, *following)
            back(0, dgu)
            back(1, dgu_next)

        loop(NT, tile)
        gradients.put_down(i, i // 2, dot_tn(act_ref[...], dy_ref[...]))
        after_down(i)
        gatherer.follow("x0/f2", i)
        when(i + 1 < NC)(lambda: start(*weights(i + 1)))
        when(i == 0)(turned.wait)
        gradients.put_wide(i, dot(aT_ref[...], dgu_ref[...]))
        after_wide(i)

    loop(NC, chunk)
    loop(n_blocks, lambda t: load(t).start())

    def store(t):
        rows = block(t, ROWS)
        return local(dy_ref.at[rows, :], dh_hbm.at[rows, :], hsem.at[t])

    def norm_back(t):
        rows = block(t, ROWS)
        load(t).wait()
        w = wide(a_ref[rows, :])
        da = wide(da_ref[rows, :].astype(bf16))
        scale = norm_scale(w)
        along = jnp.sum(da * w, -1, keepdims=True) * (scale * scale * scale) * (1.0 / D)
        dy_ref[rows, :] = (wide(dy_ref[rows, :]) + (da * scale - w * along)).astype(bf16)
        store(t).start()
        branch(t == n_blocks // 2)(lambda: gradients.wide4(NC - 2))

    gradients.wide4(NC - 3)
    loop(n_blocks, norm_back)
    sq[...] = gradients.squares()
    done = local(sq, sq_hbm, qsem)
    done.start()
    loop(n_blocks, lambda t: store(t).wait())
    gradients.finish()
    gatherer.finish()
    wait(wide_over, down_over)
    done.wait()


def last_kernel(aT_hbm, dy_hbm, kept_hbm, wd_hbm, sq_in, wide_left, down_left, eg_in, eu_in, ed_in, gg_hbm, gu_hbm, gd_hbm, sq_hbm, eg_hbm, eu_hbm, ed_hbm,
                aT_ref, dy_ref, even_dgu, even_act, odd_dgu, odd_act, by_gu, by_d, gus, wd, sq, parts, ysem, tsem, gsem, wsem, qsem, psem, left_sem, *refs):
    D, T = aT_ref.shape
    F = wd_hbm.shape[0]
    NC, NT = F // CH, T // TM
    depth = gus.shape[0]

    def states(t):
        rows = block(t, TM)
        return local(dy_hbm.at[rows, :], dy_ref.at[rows, :], ysem.at[t])

    def turned(t):
        rows = block(t, TM)
        return local(aT_hbm.at[:, rows], aT_ref.at[:, rows], tsem.at[t])

    def weights(i):
        b = odd(i)
        return rows_in(wd_hbm, wd.at[b], wsem.at[b], i)

    def kept(n):
        return local(kept_hbm.at[n // NT, block(n % NT, TM), :], gus.at[n % depth], gsem.at[n % depth])

    start(*weights(0), states(0), kept(0))
    before = local(sq_in, sq, qsem)
    before.start()
    place = Place()
    gradients = Gradients(place, refs, (gg_hbm, gu_hbm, gd_hbm), NC + 1, NC // 2 + 1, (eg_hbm, eu_hbm, ed_hbm))
    left = [local(x, r.all.at[0], left_sem.at[n]) for n, (x, r) in enumerate(((wide_left, gradients.wide), (down_left, gradients.down)))]
    start(*left)
    place.barrier(all_peers=True)

    def add(ref, term, fresh):
        ref[...] = (ref[...] if fresh is None else jnp.where(fresh, 0.0, ref[...])) + term

    def terms_gu(t, dgu_ref, fresh=None):
        add(by_gu, dot(aT_ref[:, block(t, TM)], dgu_ref[...]), fresh)

    def terms_d(t, act_ref, fresh=None):
        add(by_d, dot_tn(act_ref[...], dy_ref[block(t, TM), :]), fresh)

    def ended(i):
        q = i // 2 + 1
        gradients.put_down(i, q, by_d[...])
        gradients.put_wide(i + 1, by_gu[...])
        gradients.wide_send(i + 1)
        branch(odd(i) == 1)(lambda: gradients.down_send(q))

    def step(n, now, before):
        some = before is not None
        i, t = n // NT, n % NT
        q = i // 2

        def load_states():
            when(n < NT)(lambda: states(t).wait())
            if some:
                turned(n - 1).wait()
            when(n + 1 < NT)(lambda: start(states(n + 1)))
            when(n < NT)(lambda: start(turned(n)))
            when(n + 1 < depth)(lambda: kept(n + 1).start())

        branch(n <= NT)(load_states)

        def next_weights():
            wait(*weights(i))
            when(i + 1 < NC)(lambda: start(*weights(i + 1)))

        branch(t == 0)(next_weights)
        kept(n).wait()
        last = (t + NT - 1) % NT
        fresh = last == 0 if before is evens else None

        def dots(k):
            return dot_nt(dy_ref[block(2 * t + k, SUB), :], wd[odd(i)])

        def elementwise(k, dact):
            rows = block(k, SUB)
            silu_back(dact, gus[n % depth, rows, block(0, CH)], gus[n % depth, rows, block(1, CH)], now[1], now[0], rows)

        dact = dots(0)
        if some:
            terms_d(last, before[1], fresh)
        following = dots(1)
        elementwise(0, dact)
        if some:
            terms_gu(last, before[0], fresh)
        elementwise(1, following)
        when(n + depth < NC * NT)(lambda: kept(n + depth).start())

        def first_point():
            branch(both(odd(i) == 0, i >= 2))(lambda: gradients.down4(q - 1))
            branch(i >= 1)(lambda: ended(i - 1))
            branch(odd(i) == 1)(lambda: gradients.down2(q))

        def second_point():
            gradients.wide1(i)
            branch(i >= 1)(lambda: gradients.wide3(i - 1))

        def third_point():
            branch(odd(i) == 0)(lambda: gradients.down1(q))
            branch(odd(i) == 1)(lambda: gradients.down3(q))

        def fourth_point():
            gradients.wide2(i)
            branch(i >= 1)(lambda: gradients.wide4(i - 1))

        if some:
            for turn_at, act in enumerate((first_point, second_point, third_point, fourth_point)):
                branch(t == turn_at)(act)

    evens, odds = (even_dgu, even_act), (odd_dgu, odd_act)

    def two_steps(p):
        step(2 * p + 1, odds, evens)
        step(2 * p + 2, evens, odds)

    step(0, evens, None)
    wait(*left)
    gradients.wide_send(0)
    gradients.down_send(0)
    loop(NC * NT // 2 - 1, two_steps)
    step(NC * NT - 1 + place.s * 0, odds, evens)
    end, q = NC, NC // 2
    terms_d(NT - 1, odd_act)
    gradients.down4(q - 1)
    gradients.put_down(NC - 1, q, by_d[...])
    gradients.down_send(q)
    terms_gu(NT - 1, odd_dgu)
    gradients.put_wide(end, by_gu[...])
    gradients.wide_send(end)
    gradients.down1(q)
    gradients.wide3(end - 1)
    gradients.wide1(end)
    gradients.down2(q)
    gradients.wide4(end - 1)
    gradients.wide2(end)
    gradients.down3(q)
    gradients.wide3(end)
    before.wait()
    gradients.down4(q)
    gradients.wide4(end)
    sq[...] += gradients.squares()
    exchanges = [remote(sq, parts.at[n], psem.at[0, n], psem.at[1, n], {"s": s}) for n, s in enumerate(place.peers)]
    start(*exchanges)
    wait(*exchanges)
    sq[...] += sum(parts[n] for n in range(len(exchanges)))
    done = local(sq, sq_hbm, qsem)
    done.start()
    gradients.finish()
    done.wait()


def call(kernel, number, outs, scratch, inputs, aliases=None):
    return pl.pallas_call(
        kernel,
        out_shape=[jax.ShapeDtypeStruct(*o) for o in outs],
        in_specs=[ANY] * len(inputs),
        out_specs=[ANY] * len(outs),
        scratch_shapes=scratch,
        input_output_aliases=aliases or {},
        compiler_params=pltpu.CompilerParams(vmem_limit_bytes=VMEM_LIMIT, has_side_effects=True, collective_id=number),
    )(*inputs)


def forward(h, wg, wu, wd):
    (T, D), F = h.shape, wg.shape[2]
    chunks, down, states, turned = ((F // CH, D, BOTH), bf16), ((F, D), bf16), ((T, D), bf16), ((D, T), bf16)
    return call(
        forward_kernel,
        1,
        [((F // CH, T, BOTH), f32), states, states, turned, turned, down, chunks, down],
        [V(*states), V((T, F), bf16), V(*chunks), V(*down), V((2, D // 8, BOTH), bf16), V((2 * UNIT, D), bf16)]
        + [V((2, 2 * TM, BOTH), f32), V((2, D, ROWS), bf16), *[V(TWO + size, bf16) for size in [(SUB, D)] * 3 + [(D, SUB)]]]
        + [DMA((T // ROWS,)), DMA(TWO), DMA(TWO), DMA(TWO), DMA(TWO_THREE), DMA(())]
        + Gatherer.scratch(15),
        (h, wg, wu, wd),
    )


def middle(h, a, aT, dy, wg, wu, wd, chunks, down):
    (T, D), F = h.shape, wg.shape[2]
    mine, states = ((D // 8, F), bf16), ((T, D), bf16)
    return call(
        middle_kernel,
        2,
        [mine, mine, ((F // 8, D), bf16), states, (SMALL, f32)]
        + [((2, 4, 2) + size, bf16) for size in ((D // 8, CH), (HALF, D))]
        + [(chunks.shape, bf16), (down.shape, bf16)],
        [V(*states), V((D, T), bf16), V(*states), V((T, D), f32), V((T, BOTH), bf16), V((T, CH), bf16)]
        + [V((2, D, BOTH), bf16), V((2, CH, D), bf16), V(SMALL, f32), V((8, D // 8, BOTH), bf16), V((3 * UNIT, D), bf16)]
        + [DMA((T // ROWS,)), DMA((T // TM,)), DMA((T // TM,)), DMA(()), DMA(TWO_THREE), DMA(()), DMA(TWO)]
        + Gatherer.scratch(6)
        + Gradients.scratch(D // 8, D, F // CH // 2 - 1),
        (h, a, aT, dy, wg, wu, wd, chunks, down),
        {7: 7, 8: 8},
    )


def last(aT, dy, kept, wd, squares, wide_left, down_left, early):
    (D, T), F = aT.shape, wd.shape[0]
    mine = ((D // 8, F), bf16)
    return call(
        last_kernel,
        3,
        [mine, mine, ((F // 8, D), bf16), (SMALL, f32)] + [(g.shape, bf16) for g in early],
        [V((D, T), bf16), V((T, D), bf16), V((TM, BOTH), bf16), V((TM, CH), bf16), V((TM, BOTH), bf16), V((TM, CH), bf16), V((D, BOTH), f32), V((CH, D), f32)]
        + [V((3, TM, BOTH), f32), V((2, CH, D), bf16), V(SMALL, f32), V((7,) + SMALL, f32)]
        + [DMA((T // TM,)), DMA((T // TM,)), DMA((3,)), DMA((2, 2)), DMA(()), DMA((2, 7)), DMA(TWO)]
        + Gradients.scratch(D // 8, D, F // CH // 2 + 1),
        (aT, dy, kept, wd, squares, wide_left, down_left, *early),
        dict(zip(range(7, 10), range(4, 7))),
    )


def adamw(w, m, v, g):
    m = 0.9 * m + 0.1 * g
    v = 0.95 * v + 0.05 * g * g
    step = m * lax.rsqrt(v + 1e-8) + 0.1 * w
    return (w - 0.02 * step).astype(bf16), m, v


def update_kernel(count, sq_hbm, *refs):
    sources, targets, buffers, (sq, in_sem, out_sem, sq_sem) = refs[:15], refs[15:24], refs[24:36], refs[36:]
    units = [(layer, k) for layer in PAIR for k in range(3)]

    def buffer(which, layer, k):
        return buffers[3 * which + k].at[layer]

    def loads(layer, k):
        hbm = [sources[6 + 3 * which + k].at[layer] for which in range(3)] + [sources[3 * layer + k]]
        return [local(source, buffer(which, layer, k), in_sem.at[which, layer, k]) for which, source in enumerate(hbm)]

    def stores(layer, k):
        return [local(buffer(which, layer, k), targets[3 * which + k].at[layer], out_sem.at[which, layer, k]) for which in range(3)]

    size = local(sq_hbm, sq, sq_sem)
    size.start()
    for unit in units:
        start(*loads(*unit))
    size.wait()
    factor = jnp.minimum(1.0, 0.5 * lax.rsqrt(jnp.full((1, 1), jnp.sum(sq[...]) / count + 1e-30, f32)))
    for unit in units:
        wait(*loads(*unit))
        w, m, v, g = (buffer(which, *unit) for which in range(4))

        def take_step(t):
            rows = block(t, 16)
            w[rows, :], m[rows, :], v[rows, :] = adamw(wide(w[rows, :]), m[rows, :], v[rows, :], wide(g[rows, :]) * factor)

        loop(w.shape[0] // 16, take_step)
        start(*stores(*unit))
    for unit in units:
        wait(*stores(*unit))


def update(squares, count, firsts, seconds, weights, m, v):
    shapes = [jax.ShapeDtypeStruct(w.shape, kind) for kind in (bf16, f32, f32) for w in weights]
    return pl.pallas_call(
        functools.partial(update_kernel, count),
        out_shape=shapes,
        in_specs=[ANY] * 16,
        out_specs=[ANY] * len(shapes),
        scratch_shapes=[V(x.shape, x.dtype) for x in shapes + shapes[:3]] + [V(SMALL, f32), DMA((4, 2, 3)), DMA((3, 2, 3)), DMA(())],
        compiler_params=pltpu.CompilerParams(vmem_limit_bytes=VMEM_LIMIT),
    )(squares, *firsts, *seconds, *weights, *m, *v)


def solution(mesh):
    def step(x, dy, *arrays):
        weights, m, v = (arrays[i : i + 3] for i in (0, 3, 6))
        kept, h, a1, a1T, a0T, down0, chunks1, down1 = forward(x[0], *weights)
        *early, by_h, squares, wide_left, down_left, _, _ = middle(h, a1, a1T, dy[0], *weights, chunks1, down1)
        *first_sums, squares, gate1, up1, down_1 = last(a0T, by_h, kept, down0, squares, wide_left, down_left, early)
        count = lax.psum(1, "s") * sum(w.size for w in weights)
        return tuple(update(squares, count, first_sums, (gate1, up1, down_1), weights, m, v))

    states, cut = P(("rep", "r", "s"), None, None), P(None, "s", None)
    return jax.shard_map(
        step,
        mesh=mesh,
        in_specs=(states, states) + (cut,) * 9,
        out_specs=(P("rep", "s", None),) * 9,
        check_vma=False,
    )
```
